256 devices in a mesh: ens: 4 (over y), fsdp: 16 (over z, core), model: 4 (over x).
Axes of the slice: x: 4, y: 4, z: 8, core: 2. Of those that a mesh axis runs over, the one named last changes fastest.
Arguments:
- weight_gate: bfloat16 [8192, 8192], P(('ens', 'fsdp'), 'model'), parts along dimension 0, may hold values from -0.125 to 0.125
- low_gate: bfloat16 [8192, 32], P(('ens', 'fsdp')), parts along dimension 0, may hold values from -0.125 to 0.125
- high_gate: bfloat16 [128, 8192], P('ens', 'model'), parts along dimension 0, may hold values from -1 to 1
- weight_up: bfloat16 [8192, 8192], P(('ens', 'fsdp'), 'model'), parts along dimension 0, may hold values from -0.125 to 0.125
- low_up: bfloat16 [8192, 32], P(('ens', 'fsdp')), parts along dimension 0, may hold values from -0.125 to 0.125
- high_up: bfloat16 [128, 8192], P('ens', 'model'), parts along dimension 0, may hold values from -1 to 1
- norm_train: float32 [8192], P(('ens', 'fsdp', 'model')), parts along dimension 0, may hold values from 0.25 to 1.75
- norm_step: float32 [8192], P(('ens', 'fsdp', 'model')), parts along dimension 0, may hold values from -0.3 to 0.3
Outputs:
- final_gate: bfloat16 [32768, 2048], P(('ens', 'model')), parts along dimension 0
- final_up: bfloat16 [32768, 2048], P(('ens', 'model')), parts along dimension 0
- serve_norm: bfloat16 [8192], P('ens'), parts along dimension 0
The draws below stay inside these ranges and needn't reach their ends.
There are 4 independent parts, one for each index of `ens`. The reference program is written for one: setup_inputs(seed, part) draws one part's arguments, and reference() takes and returns one part's arrays. A program takes and returns all parts, laid end to end along the dimension named above; each array names one. Nothing has to cross between parts.
All inputs are finite; a program needn't handle non-finite values.
Results may differ from the reference program's by a relative error of at most 0.001.
Values may be sent and summed in bfloat16 or wider, within the bound.
A program may use at most 128 MiB of HBM per device.

```python
import jax
import jax.numpy as jnp

D_MODEL = 2048
D_INNER = 8192
RANK = 32


def steps_of(own_key, shape, cuts, least, high):
    def one(dim, blocks):
        steps = jax.random.uniform(jax.random.fold_in(jax.random.fold_in(own_key, 6), dim), (blocks,), jnp.float32, least / len(cuts), high / len(cuts))
        return jnp.repeat(jnp.exp(steps), shape[dim] // blocks).reshape((-1,) + (1,) * (len(shape) - dim - 1))

    gain = one(*cuts[0])
    for cut in cuts[1:]:
        gain = gain * one(*cut)
    return gain


def bell_draw(own_key, shape, spread, limit, shards=(), held_as=jnp.bfloat16):
    loudness = steps_of(own_key, shape, shards, -0.22, 0.18) if shards else 1.0
    values = jax.random.normal(own_key, shape, jnp.float32) * spread * loudness
    return jnp.minimum(jnp.maximum(values, -limit), limit).astype(held_as)


def setup_inputs(seed: int = 0, part: int = 0) -> dict:
    keys = jax.random.split(jax.random.key(seed), 9)
    part_keys = jax.random.split(jax.random.fold_in(keys[8], part), 9)
    weight_gate = bell_draw(part_keys[0], (D_MODEL, D_INNER), D_MODEL ** -0.5, 0.125, ((0, 16), (1, 4)))
    low_gate = bell_draw(part_keys[1], (D_MODEL, RANK), D_MODEL ** -0.5, 0.125, ((0, 16),))
    high_gate = bell_draw(part_keys[2], (RANK, D_INNER), RANK ** -0.5, 1.0, ((1, 4),))
    weight_up = bell_draw(part_keys[3], (D_MODEL, D_INNER), D_MODEL ** -0.5, 0.125, ((0, 16), (1, 4)))
    low_up = bell_draw(part_keys[4], (D_MODEL, RANK), D_MODEL ** -0.5, 0.125, ((0, 16),))
    high_up = bell_draw(part_keys[5], (RANK, D_INNER), RANK ** -0.5, 1.0, ((1, 4),))
    norm_train = jnp.clip(1.0 + 0.15 * jax.random.normal(part_keys[6], (D_MODEL,), jnp.float32), 0.25, 1.75)
    norm_step = jnp.clip(jax.random.uniform(part_keys[7], (D_MODEL,), jnp.float32, -0.3, 0.3) * steps_of(part_keys[7], (D_MODEL,), ((0, 64),), -0.4, 0.0), -0.3, 0.3)
    return {"weight_gate": weight_gate, "low_gate": low_gate, "high_gate": high_gate, "weight_up": weight_up, "low_up": low_up, "high_up": high_up, "norm_train": norm_train, "norm_step": norm_step}


mix_rate = 2.0


def reference(weight_gate, low_gate, high_gate, weight_up, low_up, high_up, norm_train, norm_step):
    result_gate = weight_gate.astype(jnp.float32) + mix_rate * jnp.dot(low_gate, high_gate, preferred_element_type=jnp.float32)
    result_up = weight_up.astype(jnp.float32) + mix_rate * jnp.dot(low_up, high_up, preferred_element_type=jnp.float32)
    final_gate = result_gate.T.astype(jnp.bfloat16)
    final_up = result_up.T.astype(jnp.bfloat16)
    serve_norm = (norm_train + norm_step).astype(jnp.bfloat16)
    return final_gate, final_up, serve_norm
```

```python
import functools

import jax
import jax.numpy as jnp
from jax import lax
from jax.experimental import pallas as pl
from jax.experimental.pallas import tpu as pltpu
from jax.sharding import PartitionSpec as P

mix_rate = 2.0
MESH = pl.DeviceIdType.MESH
UP, DOWN = 0, 1
GATE, RISE, NORM = 0, 1, 2
LANES = 128
PIECES = 4
HOPS = {UP: (4, 3, 4), DOWN: (3, 4, 3)}
ORDER = (
    [(GATE, 0), (GATE, 1), (NORM, 0)]
    + [(GATE, p) for p in range(2, PIECES)]
    + [(RISE, p) for p in range(PIECES)]
)
PLACE = {piece: i for i, piece in enumerate(ORDER)}


def gather_kernel(
    chips, wg, lg, hg, wu, lu, hu, nt, ns, og, ou, nb,
    wv, lv, hv, ntv, nsv, xb, in_sem, send_sem, recv_sem, sib_sem, x_sem,
):
    f = lax.axis_index("fsdp")
    m = lax.axis_index("model")
    models = lax.axis_size("model")
    z, core = f // 2, f % 2
    to = {
        UP: lax.rem(z + 1, chips) * 2 + core,
        DOWN: lax.rem(z + chips - 1, chips) * 2 + core,
    }
    sibling = z * 2 + (1 - core)
    width = wg.shape[1]
    rows = width // PIECES

    loads = []
    for k, (src, dst) in enumerate(
        (
            (lg, lv.at[0]), (hg, hv.at[0]), (wg, wv.at[0]),
            (lu, lv.at[1]), (hu, hv.at[1]), (wu, wv.at[1]),
            (nt, ntv), (ns, nsv),
        )
    ):
        load = pltpu.make_async_copy(src, dst, in_sem.at[k])
        load.start()
        loads.append(load)

    barrier = pltpu.get_barrier_semaphore()
    for peer in (to[UP], to[DOWN], sibling):
        pl.semaphore_signal(
            barrier, inc=1, device_id={"fsdp": peer}, device_id_type=MESH
        )
    for k in range(1, models):
        pl.semaphore_signal(
            barrier, inc=1, device_id={"model": lax.rem(m + k, models)}, device_id_type=MESH
        )

    def piece_of(kind, p, owner):
        if kind == NORM:
            return nb.at[pl.ds(owner, 1)]
        out = og if kind == GATE else ou
        lanes = pl.ds(pl.multiple_of(owner * LANES, LANES), LANES)
        return out.at[pl.ds(p * rows, rows), lanes]

    def push(kind, p, owner):
        ref = piece_of(kind, p, owner)
        pltpu.make_async_remote_copy(
            src_ref=ref, dst_ref=ref, send_sem=send_sem.at[2, kind], recv_sem=sib_sem.at[kind],
            device_id={"fsdp": sibling}, device_id_type=MESH,
        ).start()

    def hop(way, step, kind, p, owner):
        ref = piece_of(kind, p, owner)
        return pltpu.make_async_remote_copy(
            src_ref=ref, dst_ref=ref, send_sem=send_sem.at[way, kind],
            recv_sem=recv_sem.at[way, step - 1, PLACE[kind, p]],
            device_id={"fsdp": to[way]}, device_id_type=MESH,
        )

    def send_own(kind, p):
        for way in (UP, DOWN):
            hop(way, 1, kind, p, f).start()
        push(kind, p, f)

    def merge(kind, p):
        columns = pl.ds(p * rows, rows)
        low_high = lax.dot_general(
            lv[kind], hv[kind, :, columns], (((0,), (0,)), ((), ())),
            preferred_element_type=jnp.float32,
        )
        result = wv[kind, :, columns].astype(jnp.float32) + mix_rate * low_high
        piece_of(kind, p, f)[...] = result.T.astype(jnp.bfloat16)

    for k in range(3):
        loads[k].wait()
    merge(GATE, 0)
    loads[6].wait()
    loads[7].wait()
    xb[m] = jnp.zeros((1, LANES), jnp.float32)
    xb[m, :, pl.ds(0, nt.shape[0])] = (ntv[...] + nsv[...]).reshape(1, nt.shape[0])
    merge(GATE, 1)
    pl.semaphore_wait(barrier, 3 + models - 1)
    x_copies = []
    for k in range(1, models):
        copy = pltpu.make_async_remote_copy(
            src_ref=xb.at[m], dst_ref=xb.at[m], send_sem=x_sem.at[0], recv_sem=x_sem.at[1],
            device_id={"model": lax.rem(m + k, models)}, device_id_type=MESH,
        )
        copy.start()
    send_own(GATE, 0)
    send_own(GATE, 1)
    merge(GATE, 2)
    merge(GATE, 3)
    for k in range(3, 6):
        loads[k].wait()
    merge(RISE, 0)
    others = xb.at[pl.ds(0, models - 1)]
    pltpu.make_async_copy(others, others, x_sem.at[1]).wait()
    lane = lax.broadcasted_iota(jnp.int32, (1, LANES), 1)
    part = LANES // models
    row = xb[0]
    for k in range(1, models):
        row = jnp.where(lane >= k * part, pltpu.roll(xb[k], k * part, 1), row)
    nb[f] = row
    merge(RISE, 1)
    send_own(NORM, 0)
    send_own(GATE, 2)
    send_own(GATE, 3)
    send_own(RISE, 0)
    merge(RISE, 2)
    send_own(RISE, 1)
    merge(RISE, 3)
    send_own(RISE, 2)
    pltpu.make_async_copy(others, others, x_sem.at[0]).wait()
    send_own(RISE, 3)

    arrivals = {
        way: [
            (step, kind, p)
            for step in range(1, 5)
            for kind, p in ORDER
            if step <= HOPS[way][kind]
        ]
        for way in (UP, DOWN)
    }
    for i in range(max(len(a) for a in arrivals.values())):
        for way in (UP, DOWN):
            if i >= len(arrivals[way]):
                continue
            step, kind, p = arrivals[way][i]
            back = chips - step if way == UP else step
            owner = lax.rem(z + back, chips) * 2 + core
            hop(way, step, kind, p, owner).wait_recv()
            if step < HOPS[way][kind]:
                hop(way, step + 1, kind, p, owner).start()
            push(kind, p, owner)

    for kind, out in ((NORM, nb), (GATE, og), (RISE, ou)):
        unit = out.shape[0] // (2 * chips)
        for sem, blocks in (
            (sib_sem.at[kind], chips),
            (send_sem.at[UP, kind], HOPS[UP][kind]),
            (send_sem.at[DOWN, kind], HOPS[DOWN][kind]),
            (send_sem.at[2, kind], chips),
        ):
            ref = out.at[pl.ds(0, unit * blocks)]
            pltpu.make_async_copy(ref, ref, sem).wait()


def write_kernel(og, ou, nb, fg, fu, fn, sem):
    copies = []
    cuts = 4
    for k, (src, dst) in enumerate(((og, fg), (ou, fu))):
        rows = src.shape[0] // cuts
        for c in range(cuts):
            cut = pl.ds(c * rows, rows)
            copy = pltpu.make_async_copy(src.at[cut], dst.at[cut], sem.at[k * cuts + c])
            copy.start()
            copies.append(copy)
    fn[...] = nb[...].reshape(fn.shape).astype(fn.dtype)
    for copy in copies:
        copy.wait()


def solution(mesh):
    fsdp = mesh.shape["fsdp"]
    models = mesh.shape["model"]
    chips = fsdp // 2

    def body(wg, lg, hg, wu, lu, hu, nt, ns):
        depth, width = wg.shape
        rank = lg.shape[1]
        model_width = depth * fsdp
        anywhere = pl.BlockSpec(memory_space=pl.ANY)
        on_chip = pl.BlockSpec(memory_space=pltpu.VMEM)
        og, ou, nb = pl.pallas_call(
            functools.partial(gather_kernel, chips),
            out_shape=(
                pltpu.VMEM((width, model_width), jnp.bfloat16),
                pltpu.VMEM((width, model_width), jnp.bfloat16),
                pltpu.VMEM((fsdp, 1, LANES), jnp.float32),
            ),
            in_specs=[pl.BlockSpec(memory_space=pltpu.HBM)] * 8,
            out_specs=(on_chip,) * 3,
            scratch_shapes=[
                pltpu.VMEM((2, depth, width), jnp.bfloat16),
                pltpu.VMEM((2, rank, depth), jnp.bfloat16),
                pltpu.VMEM((2, rank, width), jnp.bfloat16),
                pltpu.VMEM(nt.shape, jnp.float32),
                pltpu.VMEM(ns.shape, jnp.float32),
                pltpu.VMEM((models, 1, LANES), jnp.float32),
                pltpu.SemaphoreType.DMA((8,)),
                pltpu.SemaphoreType.DMA((3, 3)),
                pltpu.SemaphoreType.DMA((2, 4, len(ORDER))),
                pltpu.SemaphoreType.DMA((3,)),
                pltpu.SemaphoreType.DMA((2,)),
            ],
            compiler_params=pltpu.CompilerParams(
                collective_id=0, has_side_effects=True, vmem_limit_bytes=50257920
            ),
            name="gather",
        )(wg, lg.T, hg, wu, lu.T, hu, nt, ns)
        fg, fu, fn = pl.pallas_call(
            write_kernel,
            out_shape=(
                jax.ShapeDtypeStruct((width, model_width), jnp.bfloat16),
                jax.ShapeDtypeStruct((width, model_width), jnp.bfloat16),
                jax.ShapeDtypeStruct((fsdp, LANES), jnp.bfloat16),
            ),
            in_specs=[on_chip] * 3,
            out_specs=(anywhere, anywhere, on_chip),
            scratch_shapes=[pltpu.SemaphoreType.DMA((8,))],
            compiler_params=pltpu.CompilerParams(vmem_limit_bytes=20 << 20),
            name="write",
        )(og, ou, nb)
        return fg, fu, fn.reshape(fsdp * LANES)

    return jax.shard_map(
        body,
        mesh=mesh,
        in_specs=(
            P(("ens", "fsdp"), "model"),
            P(("ens", "fsdp"), None),
            P("ens", "model"),
            P(("ens", "fsdp"), "model"),
            P(("ens", "fsdp"), None),
            P("ens", "model"),
            P(("ens", "fsdp", "model")),
            P(("ens", "fsdp", "model")),
        ),
        out_specs=(P(("ens", "model"), None), P(("ens", "model"), None), P("ens")),
        check_vma=False,
    )
```

```python
import functools

import jax
import jax.numpy as jnp
from jax import lax
from jax.experimental import pallas as pl
from jax.experimental.pallas import tpu as pltpu
from jax.sharding import PartitionSpec as P

mix_rate = 2.0
MESH = pl.DeviceIdType.MESH
UP, DOWN = 0, 1
GATE, RISE, NORM = 0, 1, 2
LANES = 128
CUTS = {GATE: (256, 512, 512, 512, 128, 128), RISE: (512, 512, 512, 256, 128, 128), NORM: (1,)}
HOPS = {UP: (4, 3, 4), DOWN: (3, 4, 3)}
ORDER = [(GATE, p) for p in range(len(CUTS[GATE]))] + [(RISE, p) for p in range(len(CUTS[RISE]))]
ORDER.insert(3, (NORM, 0))
PLACE = {piece: i for i, piece in enumerate(ORDER)}


def gather_kernel(
    chips, wg, lg, hg, wu, lu, hu, nt, ns, og, ou, nb,
    wv, lv, hv, ntv, nsv, xb, in_sem, send_sem, recv_sem, sib_sem, x_sem,
):
    f = lax.axis_index("fsdp")
    m = lax.axis_index("model")
    models = lax.axis_size("model")
    z, core = f // 2, f % 2
    to = {
        UP: lax.rem(z + 1, chips) * 2 + core,
        DOWN: lax.rem(z + chips - 1, chips) * 2 + core,
    }
    sibling = z * 2 + (1 - core)

    loads = []
    for k, (src, dst) in enumerate(
        (
            (lg, lv.at[0]), (hg, hv.at[0]), (wg, wv.at[0]),
            (lu, lv.at[1]), (hu, hv.at[1]), (wu, wv.at[1]),
            (nt, ntv), (ns, nsv),
        )
    ):
        load = pltpu.make_async_copy(src, dst, in_sem.at[k])
        load.start()
        loads.append(load)

    barrier = pltpu.get_barrier_semaphore()
    for peer in (to[UP], to[DOWN], sibling):
        pl.semaphore_signal(
            barrier, inc=1, device_id={"fsdp": peer}, device_id_type=MESH
        )
    for k in range(1, models):
        pl.semaphore_signal(
            barrier, inc=1, device_id={"model": lax.rem(m + k, models)}, device_id_type=MESH
        )

    def rows_of(kind, p):
        return pl.ds(sum(CUTS[kind][:p]), CUTS[kind][p])

    def piece_of(kind, p, owner):
        if kind == NORM:
            return nb.at[pl.ds(owner, 1)]
        out = og if kind == GATE else ou
        lanes = pl.ds(pl.multiple_of(owner * LANES, LANES), LANES)
        return out.at[rows_of(kind, p), lanes]

    def push(kind, p, owner):
        ref = piece_of(kind, p, owner)
        pltpu.make_async_remote_copy(
            src_ref=ref, dst_ref=ref, send_sem=send_sem.at[2, kind], recv_sem=sib_sem.at[kind],
            device_id={"fsdp": sibling}, device_id_type=MESH,
        ).start()

    def hop(way, step, kind, p, owner):
        ref = piece_of(kind, p, owner)
        return pltpu.make_async_remote_copy(
            src_ref=ref, dst_ref=ref, send_sem=send_sem.at[way, kind],
            recv_sem=recv_sem.at[way, step - 1, PLACE[kind, p]],
            device_id={"fsdp": to[way]}, device_id_type=MESH,
        )

    def send_own(kind, p):
        for way in (UP, DOWN):
            hop(way, 1, kind, p, f).start()
        push(kind, p, f)

    def merge(kind, p):
        columns = rows_of(kind, p)
        low_high = lax.dot_general(
            lv[kind], hv[kind, :, columns], (((0,), (0,)), ((), ())),
            preferred_element_type=jnp.float32,
        )
        result = wv[kind, :, columns].astype(jnp.float32) + mix_rate * low_high
        piece_of(kind, p, f)[...] = result.T.astype(jnp.bfloat16)

    others = xb.at[pl.ds(0, models - 1)]
    lane = lax.broadcasted_iota(jnp.int32, (1, LANES), 1)
    part = LANES // models

    def norm_part():
        loads[6].wait()
        loads[7].wait()
        xb[m] = jnp.zeros((1, LANES), jnp.float32)
        xb[m, :, pl.ds(0, part)] = (ntv[...] + nsv[...]).reshape(1, part)

    def norm_exchange():
        for k in range(1, models):
            pltpu.make_async_remote_copy(
                src_ref=xb.at[m], dst_ref=xb.at[m], send_sem=x_sem.at[0], recv_sem=x_sem.at[1],
                device_id={"model": lax.rem(m + k, models)}, device_id_type=MESH,
            ).start()

    def norm_row():
        pltpu.make_async_copy(others, others, x_sem.at[1]).wait()
        row = xb[0]
        for k in range(1, models):
            row = jnp.where(lane >= k * part, pltpu.roll(xb[k], k * part, 1), row)
        nb[f] = row

    for k in range(3):
        loads[k].wait()
    merge(GATE, 0)
    norm_part()
    pl.semaphore_wait(barrier, 3 + models - 1)
    send_own(GATE, 0)
    norm_exchange()
    made = [piece for piece in ORDER if piece[0] != NORM]
    pending = []
    for i, piece in enumerate(made[1:]):
        if piece == (RISE, 0):
            for k in range(3, 6):
                loads[k].wait()
            norm_row()
            pending.insert(0, (NORM, 0))
        merge(*piece)
        pending.append(piece)
        if piece[0] == GATE and piece[1] < 3:
            if len(pending) > 1:
                send_own(*pending.pop(0))
        elif piece[0] == RISE:
            while len(pending) > 1:
                send_own(*pending.pop(0))
    pltpu.make_async_copy(others, others, x_sem.at[0]).wait()
    while pending:
        send_own(*pending.pop(0))

    arrivals = {
        way: [
            (step, kind, p)
            for step in range(1, 5)
            for kind, p in ORDER
            if step <= HOPS[way][kind]
        ]
        for way in (UP, DOWN)
    }
    for i in range(max(len(a) for a in arrivals.values())):
        for way in (UP, DOWN):
            if i >= len(arrivals[way]):
                continue
            step, kind, p = arrivals[way][i]
            back = chips - step if way == UP else step
            owner = lax.rem(z + back, chips) * 2 + core
            hop(way, step, kind, p, owner).wait_recv()
            if step < HOPS[way][kind]:
                hop(way, step + 1, kind, p, owner).start()
            push(kind, p, owner)

    for kind, out in ((NORM, nb), (GATE, og), (RISE, ou)):
        unit = out.shape[0] // (2 * chips)
        for sem, blocks in (
            (sib_sem.at[kind], chips),
            (send_sem.at[UP, kind], HOPS[UP][kind]),
            (send_sem.at[DOWN, kind], HOPS[DOWN][kind]),
            (send_sem.at[2, kind], chips),
        ):
            ref = out.at[pl.ds(0, unit * blocks)]
            pltpu.make_async_copy(ref, ref, sem).wait()


def write_kernel(og, ou, nb, fg, fu, fn, norm, sem):
    norm[...] = nb[...].reshape(norm.shape).astype(norm.dtype)
    copies = []
    cuts = 4
    for k, (src, dst) in enumerate(((og, fg), (ou, fu))):
        rows = src.shape[0] // cuts
        for c in range(cuts):
            cut = pl.ds(c * rows, rows)
            copies.append(pltpu.make_async_copy(src.at[cut], dst.at[cut], sem.at[k * cuts + c]))
            copies[-1].start()
    copies.append(pltpu.make_async_copy(norm, fn, sem.at[2 * cuts]))
    copies[-1].start()
    for copy in copies:
        copy.wait()


def solution(mesh):
    fsdp = mesh.shape["fsdp"]
    models = mesh.shape["model"]
    chips = fsdp // 2

    def body(wg, lg, hg, wu, lu, hu, nt, ns):
        depth, width = wg.shape
        rank = lg.shape[1]
        model_width = depth * fsdp
        anywhere = pl.BlockSpec(memory_space=pl.ANY)
        on_chip = pl.BlockSpec(memory_space=pltpu.VMEM)
        og, ou, nb = pl.pallas_call(
            functools.partial(gather_kernel, chips),
            out_shape=(
                pltpu.VMEM((width, model_width), jnp.bfloat16),
                pltpu.VMEM((width, model_width), jnp.bfloat16),
                pltpu.VMEM((fsdp, 1, LANES), jnp.float32),
            ),
            in_specs=[pl.BlockSpec(memory_space=pltpu.HBM)] * 8,
            out_specs=(on_chip,) * 3,
            scratch_shapes=[
                pltpu.VMEM((2, depth, width), jnp.bfloat16),
                pltpu.VMEM((2, rank, depth), jnp.bfloat16),
                pltpu.VMEM((2, rank, width), jnp.bfloat16),
                pltpu.VMEM(nt.shape, jnp.float32),
                pltpu.VMEM(ns.shape, jnp.float32),
                pltpu.VMEM((models, 1, LANES), jnp.float32),
                pltpu.SemaphoreType.DMA((8,)),
                pltpu.SemaphoreType.DMA((3, 3)),
                pltpu.SemaphoreType.DMA((2, 4, len(ORDER))),
                pltpu.SemaphoreType.DMA((3,)),
                pltpu.SemaphoreType.DMA((2,)),
            ],
            compiler_params=pltpu.CompilerParams(
                collective_id=0, has_side_effects=True, vmem_limit_bytes=50257920
            ),
            name="gather",
        )(wg, lg.T, hg, wu, lu.T, hu, nt, ns)
        fg, fu, fn = pl.pallas_call(
            write_kernel,
            out_shape=(
                jax.ShapeDtypeStruct((width, model_width), jnp.bfloat16),
                jax.ShapeDtypeStruct((width, model_width), jnp.bfloat16),
                jax.ShapeDtypeStruct((fsdp, LANES), jnp.bfloat16),
            ),
            in_specs=[on_chip] * 3,
            out_specs=(anywhere,) * 3,
            scratch_shapes=[pltpu.VMEM((fsdp, LANES), jnp.bfloat16), pltpu.SemaphoreType.DMA((9,))],
            compiler_params=pltpu.CompilerParams(vmem_limit_bytes=20 << 20),
            name="write",
        )(og, ou, nb)
        return fg, fu, fn.reshape(fsdp * LANES)

    return jax.shard_map(
        body,
        mesh=mesh,
        in_specs=(
            P(("ens", "fsdp"), "model"),
            P(("ens", "fsdp"), None),
            P("ens", "model"),
            P(("ens", "fsdp"), "model"),
            P(("ens", "fsdp"), None),
            P("ens", "model"),
            P(("ens", "fsdp", "model")),
            P(("ens", "fsdp", "model")),
        ),
        out_specs=(P(("ens", "model"), None), P(("ens", "model"), None), P("ens")),
        check_vma=False,
    )
```

```python
import functools

import jax
import jax.numpy as jnp
from jax import lax
from jax.experimental import pallas as pl
from jax.experimental.pallas import tpu as pltpu
from jax.sharding import PartitionSpec as P

mix_rate = 2.0
MESH = pl.DeviceIdType.MESH
UP, DOWN = 0, 1
GATE, RISE, NORM = 0, 1, 2
LANES = 128
CUTS = {GATE: (256, 512, 512, 512, 128, 128), RISE: (512, 512, 512, 256, 128, 128), NORM: (1,)}
HOPS = {UP: (4, 3, 4), DOWN: (3, 4, 3)}
ORDER = [(GATE, p) for p in range(len(CUTS[GATE]))] + [(RISE, p) for p in range(len(CUTS[RISE]))]
ORDER.insert(3, (NORM, 0))
ARRIVALS = {
    way: [
        (step, kind, p)
        for step in range(1, 5)
        for kind, p in ORDER
        if step <= HOPS[way][kind]
    ]
    for way in (UP, DOWN)
}
FIRST = (27, 41)
LEAST = min(FIRST)
AHEAD = FIRST.index(LEAST)
MEET = 36


def early(core, way, step, kind, p):
    return ARRIVALS[way].index((step, kind, p)) < FIRST[core]


def shared_early(way, i):
    return i < LEAST


def position(chips):
    f = lax.axis_index("fsdp")
    z, core = f // 2, f % 2
    to = {
        UP: lax.rem(z + 1, chips) * 2 + core,
        DOWN: lax.rem(z + chips - 1, chips) * 2 + core,
    }
    return f, z, core, to, z * 2 + (1 - core)


def owner_of(chips, z, core, way, step):
    back = chips - step if way == UP else step
    return lax.rem(z + back, chips) * 2 + core


def rows_of(kind, p):
    return pl.ds(sum(CUTS[kind][:p]), CUTS[kind][p])


def lanes_of(owner):
    return pl.ds(pl.multiple_of(owner * LANES, LANES), LANES)


def piece_of(held, kind, p, owner):
    if kind == NORM:
        return held[NORM].at[pl.ds(owner, 1)]
    return held[kind].at[rows_of(kind, p), lanes_of(owner)]


def copy_to(source, target, send_sem, recv_sem, fsdp):
    return pltpu.make_async_remote_copy(
        src_ref=source, dst_ref=target, send_sem=send_sem, recv_sem=recv_sem,
        device_id={"fsdp": fsdp}, device_id_type=MESH,
    )


def wait_for(held, kind, rows, sem):
    if rows:
        ref = held[kind].at[pl.ds(0, rows if kind == NORM else rows * LANES // held[kind].shape[1])]
        pltpu.make_async_copy(ref, ref, sem).wait()


def rows_in(pieces):
    return [sum(CUTS[k][p] for k, p in pieces if k == kind) for kind in (GATE, RISE, NORM)]


def each(first, last):
    for i in range(first, last):
        for way in (UP, DOWN):
            if i < len(ARRIVALS[way]):
                yield i, way, *ARRIVALS[way][i]


COUNT = max(len(a) for a in ARRIVALS.values())


def gather_kernel(
    chips, wg, lg, hg, wu, lu, hu, nt, ns, og, ou, nb,
    wv, lv, hv, ntv, nsv, xb, in_sem, send_sem, recv_sem, sib_sem, x_sem,
):
    f, z, core, to, sibling = position(chips)
    m = lax.axis_index("model")
    models = lax.axis_size("model")
    held = (og, ou, nb)

    loads = []
    for k, (src, dst) in enumerate(
        (
            (lg, lv.at[0]), (hg, hv.at[0]), (wg, wv.at[0]),
            (lu, lv.at[1]), (hu, hv.at[1]), (wu, wv.at[1]),
            (nt, ntv), (ns, nsv),
        )
    ):
        load = pltpu.make_async_copy(src, dst, in_sem.at[k])
        load.start()
        loads.append(load)

    barrier = pltpu.get_barrier_semaphore()
    for peer in (to[UP], to[DOWN], sibling):
        pl.semaphore_signal(
            barrier, inc=1, device_id={"fsdp": peer}, device_id_type=MESH
        )
    for k in range(1, models):
        pl.semaphore_signal(
            barrier, inc=1, device_id={"model": lax.rem(m + k, models)}, device_id_type=MESH
        )

    def push(kind, p, owner):
        ref = piece_of(held, kind, p, owner)
        copy_to(ref, ref, send_sem.at[2, kind], sib_sem.at[kind], sibling).start()

    def hop(way, step, kind, p, owner):
        ref = piece_of(held, kind, p, owner)
        place = ARRIVALS[way].index((step, kind, p))
        return copy_to(ref, ref, send_sem.at[way, kind], recv_sem.at[way, place], to[way])

    def send_own(kind, p):
        for way in (UP, DOWN):
            hop(way, 1, kind, p, f).start()
        push(kind, p, f)

    def merge(kind, p):
        columns = rows_of(kind, p)
        low_high = lax.dot_general(
            lv[kind], hv[kind, :, columns], (((0,), (0,)), ((), ())),
            preferred_element_type=jnp.float32,
        )
        result = wv[kind, :, columns].astype(jnp.float32) + mix_rate * low_high
        piece_of(held, kind, p, f)[...] = result.T.astype(jnp.bfloat16)

    others = xb.at[pl.ds(0, models - 1)]
    lane = lax.broadcasted_iota(jnp.int32, (1, LANES), 1)
    part = LANES // models

    def norm_part():
        loads[6].wait()
        loads[7].wait()
        xb[m] = jnp.zeros((1, LANES), jnp.float32)
        xb[m, :, pl.ds(0, part)] = (ntv[...] + nsv[...]).reshape(1, part)

    def norm_exchange():
        for k in range(1, models):
            pltpu.make_async_remote_copy(
                src_ref=xb.at[m], dst_ref=xb.at[m], send_sem=x_sem.at[0], recv_sem=x_sem.at[1],
                device_id={"model": lax.rem(m + k, models)}, device_id_type=MESH,
            ).start()

    def norm_row():
        pltpu.make_async_copy(others, others, x_sem.at[1]).wait()
        row = xb[0]
        for k in range(1, models):
            row = jnp.where(lane >= k * part, pltpu.roll(xb[k], k * part, 1), row)
        nb[f] = row

    for k in range(3):
        loads[k].wait()
    merge(GATE, 0)
    norm_part()
    pl.semaphore_wait(barrier, 3 + models - 1)
    send_own(GATE, 0)
    norm_exchange()
    made = [piece for piece in ORDER if piece[0] != NORM]
    pending = []
    for i, piece in enumerate(made[1:]):
        if piece == (RISE, 0):
            for k in range(3, 6):
                loads[k].wait()
            norm_row()
            pending.insert(0, (NORM, 0))
        merge(*piece)
        pending.append(piece)
        if piece[0] == GATE and piece[1] < 3:
            if len(pending) > 1:
                send_own(*pending.pop(0))
        elif piece[0] == RISE:
            while len(pending) > 1:
                send_own(*pending.pop(0))
    pltpu.make_async_copy(others, others, x_sem.at[0]).wait()
    while pending:
        send_own(*pending.pop(0))

    def take(c):
        sent = {way: list(ORDER) for way in (UP, DOWN)}
        pushed = list(ORDER)
        for i, way, step, kind, p in each(0, FIRST[c]):
            owner = owner_of(chips, z, core, way, step)
            hop(way, step, kind, p, owner).wait_recv()
            if step < HOPS[way][kind] and early(c, way, step + 1, kind, p):
                hop(way, step + 1, kind, p, owner).start()
                sent[way].append((kind, p))
            if shared_early(way, i):
                push(kind, p, owner)
                pushed.append((kind, p))
        for kind in (NORM, GATE, RISE):
            for way in (UP, DOWN):
                wait_for(held, kind, rows_in(sent[way])[kind], send_sem.at[way, kind])
            wait_for(held, kind, rows_in(pushed)[kind], send_sem.at[2, kind])
            wait_for(held, kind, rows_in(pushed)[kind], sib_sem.at[kind])

    for c in (0, 1):
        pl.when(core == c)(functools.partial(take, c))


def finish_kernel(chips, og, ou, nb, after, lg, lu, ln, send_sem, recv_sem, sib_sem, ready):
    f, z, core, to, sibling = position(chips)
    before, held = (og, ou, nb), (lg, lu, ln)
    barrier = pltpu.get_barrier_semaphore()
    for peer in (to[UP], to[DOWN]):
        pl.semaphore_signal(
            barrier, inc=1, device_id={"fsdp": peer}, device_id_type=MESH
        )

    @pl.when(core == AHEAD)
    def _():
        pl.semaphore_signal(
            barrier, inc=1, device_id={"fsdp": sibling}, device_id_type=MESH
        )
        pl.semaphore_wait(barrier, 2)

    @pl.when(core != AHEAD)
    def _():
        pl.semaphore_wait(barrier, 3)
        pl.semaphore_signal(
            ready, inc=1, device_id={"fsdp": sibling}, device_id_type=MESH
        )

    def push(source, kind, p, owner):
        copy_to(
            piece_of(source, kind, p, owner), piece_of(held, kind, p, owner),
            send_sem.at[2, kind], sib_sem.at[kind], sibling,
        ).start()

    def hop(source, way, step, kind, p, owner):
        place = ARRIVALS[way].index((step, kind, p))
        return copy_to(
            piece_of(source, kind, p, owner), piece_of(held, kind, p, owner),
            send_sem.at[way, kind], recv_sem.at[way, place], to[way],
        )

    def take(c):
        sent = {way: [] for way in (UP, DOWN)}
        pushed, late = [], []
        for i, way, step, kind, p in each(0, FIRST[c]):
            owner = owner_of(chips, z, core, way, step)
            if step < HOPS[way][kind] and not early(c, way, step + 1, kind, p):
                hop(before, way, step + 1, kind, p, owner).start()
                sent[way].append((kind, p))
            if not shared_early(way, i):
                late.append((before, kind, p, way, step))

        def push_late():
            while late:
                source, kind, p, way, step = late.pop(0)
                push(source, kind, p, owner_of(chips, z, core, way, step))
                pushed.append((kind, p))

        met = c != AHEAD
        for i, way, step, kind, p in each(FIRST[c], COUNT):
            if not met and i >= MEET:
                pl.semaphore_wait(ready, 1)
                met = True
            if met:
                push_late()
            owner = owner_of(chips, z, core, way, step)
            hop(held, way, step, kind, p, owner).wait_recv()
            if step < HOPS[way][kind]:
                hop(held, way, step + 1, kind, p, owner).start()
                sent[way].append((kind, p))
            late.append((held, kind, p, way, step))
        push_late()
        coming = [(kind, p) for _, _, _, kind, p in each(LEAST, COUNT)]
        for kind in (NORM, GATE, RISE):
            for way in (UP, DOWN):
                wait_for(held, kind, rows_in(sent[way])[kind], send_sem.at[way, kind])
            wait_for(held, kind, rows_in(pushed)[kind], send_sem.at[2, kind])
            wait_for(held, kind, rows_in(coming)[kind], sib_sem.at[kind])

    for c in (0, 1):
        pl.when(core == c)(functools.partial(take, c))


def runs(pieces):
    out = []
    for kind, p in sorted(pieces):
        start, size = sum(CUTS[kind][:p]), CUTS[kind][p]
        if out and out[-1][0] == kind and sum(out[-1][1:]) == start:
            out[-1] = (kind, out[-1][1], out[-1][2] + size)
        else:
            out.append((kind, start, size))
    return out


def store(chips, z, core, c, held, final, sem, sides, own):
    total = [0, 0]
    for mine, (first, last) in ((True, sides[0]), (False, sides[1])):
        line = core if mine else 1 - core
        blocks = {}
        for _, way, step, kind, p in each(first, last):
            if kind != NORM:
                blocks.setdefault((way, step), []).append((kind, p))
        if own:
            blocks[UP, 0] = [piece for piece in ORDER if piece[0] != NORM]
        for (way, step), pieces in blocks.items():
            lanes = lanes_of(owner_of(chips, z, line, way, step))
            for kind, start, size in runs(pieces):
                at = (pl.ds(start, size), lanes)
                pltpu.make_async_copy(held[kind].at[at], final[kind].at[at], sem.at[kind]).start()
                total[kind] += size
    return total


def write_kernel(chips, og, ou, fg, fu, after, sem):
    _, z, core, _, _ = position(chips)
    after[...] = jnp.zeros_like(after)
    held, final = (og, ou), (fg, fu)

    def take(c):
        total = store(chips, z, core, c, held, final, sem, ((0, FIRST[c]), (0, LEAST)), True)
        for kind in (GATE, RISE):
            wait_for(held, kind, total[kind], sem.at[kind])

    for c in (0, 1):
        pl.when(core == c)(functools.partial(take, c))


def write_rest_kernel(chips, fg_in, fu_in, nb, lg, lu, ln, fg, fu, fn, rows, norm, sem):
    f, z, core, _, sibling = position(chips)
    held, final = (lg, lu), (fg, fu)

    def take(c):
        total = store(
            chips, z, core, c, held, final, sem, ((FIRST[c], COUNT), (LEAST, COUNT)), False
        )
        rows[f] = nb[f]
        rows[sibling] = nb[sibling]
        for i, way, step, kind, p in each(0, COUNT):
            if kind == NORM:
                for line, source in ((core, i < FIRST[c]), (1 - core, i < LEAST)):
                    owner = owner_of(chips, z, line, way, step)
                    rows[owner] = nb[owner] if source else ln[owner]
        norm[...] = rows[...].reshape(norm.shape).astype(norm.dtype)
        last = pltpu.make_async_copy(norm, fn, sem.at[2])
        last.start()
        for kind in (GATE, RISE):
            wait_for(held, kind, total[kind], sem.at[kind])
        last.wait()

    for c in (0, 1):
        pl.when(core == c)(functools.partial(take, c))


def solution(mesh):
    fsdp = mesh.shape["fsdp"]
    models = mesh.shape["model"]
    chips = fsdp // 2

    def body(wg, lg, hg, wu, lu, hu, nt, ns):
        depth, width = wg.shape
        rank = lg.shape[1]
        model_width = depth * fsdp
        anywhere = pl.BlockSpec(memory_space=pl.ANY)
        on_chip = pl.BlockSpec(memory_space=pltpu.VMEM)
        final = jax.ShapeDtypeStruct((width, model_width), jnp.bfloat16)
        on_chip_held = (
            pltpu.VMEM((width, model_width), jnp.bfloat16),
            pltpu.VMEM((width, model_width), jnp.bfloat16),
            pltpu.VMEM((fsdp, 1, LANES), jnp.float32),
        )
        ring_sems = [
            pltpu.SemaphoreType.DMA((3, 3)),
            pltpu.SemaphoreType.DMA((2, COUNT)),
            pltpu.SemaphoreType.DMA((3,)),
        ]
        og, ou, nb = pl.pallas_call(
            functools.partial(gather_kernel, chips),
            out_shape=on_chip_held,
            in_specs=[pl.BlockSpec(memory_space=pltpu.HBM)] * 8,
            out_specs=(on_chip,) * 3,
            scratch_shapes=[
                pltpu.VMEM((2, depth, width), jnp.bfloat16),
                pltpu.VMEM((2, rank, depth), jnp.bfloat16),
                pltpu.VMEM((2, rank, width), jnp.bfloat16),
                pltpu.VMEM(nt.shape, jnp.float32),
                pltpu.VMEM(ns.shape, jnp.float32),
                pltpu.VMEM((models, 1, LANES), jnp.float32),
                pltpu.SemaphoreType.DMA((8,)),
                *ring_sems,
                pltpu.SemaphoreType.DMA((2,)),
            ],
            compiler_params=pltpu.CompilerParams(
                collective_id=0, has_side_effects=True, vmem_limit_bytes=50257920
            ),
            name="gather",
        )(wg, lg.T, hg, wu, lu.T, hu, nt, ns)
        fg, fu, after = pl.pallas_call(
            functools.partial(write_kernel, chips),
            out_shape=(final, final, pltpu.VMEM((8, LANES), jnp.float32)),
            in_specs=[on_chip] * 2,
            out_specs=(anywhere, anywhere, on_chip),
            scratch_shapes=[pltpu.SemaphoreType.DMA((2,))],
            compiler_params=pltpu.CompilerParams(vmem_limit_bytes=4 << 20),
            name="write",
        )(og, ou)
        lg2, lu2, ln = pl.pallas_call(
            functools.partial(finish_kernel, chips),
            out_shape=on_chip_held,
            in_specs=[on_chip] * 4,
            out_specs=(on_chip,) * 3,
            scratch_shapes=[*ring_sems, pltpu.SemaphoreType.REGULAR],
            compiler_params=pltpu.CompilerParams(
                collective_id=1, has_side_effects=True, vmem_limit_bytes=4 << 20
            ),
            name="finish",
        )(og, ou, nb, after)
        fg, fu, fn = pl.pallas_call(
            functools.partial(write_rest_kernel, chips),
            out_shape=(final, final, jax.ShapeDtypeStruct((fsdp, LANES), jnp.bfloat16)),
            in_specs=[anywhere] * 2 + [on_chip] * 4,
            out_specs=(anywhere,) * 3,
            scratch_shapes=[
                pltpu.VMEM((fsdp, 1, LANES), jnp.float32),
                pltpu.VMEM((fsdp, LANES), jnp.bfloat16),
                pltpu.SemaphoreType.DMA((3,)),
            ],
            input_output_aliases={0: 0, 1: 1},
            compiler_params=pltpu.CompilerParams(vmem_limit_bytes=4 << 20),
            name="write_rest",
        )(fg, fu, nb, lg2, lu2, ln)
        return fg, fu, fn.reshape(fsdp * LANES)

    return jax.shard_map(
        body,
        mesh=mesh,
        in_specs=(
            P(("ens", "fsdp"), "model"),
            P(("ens", "fsdp"), None),
            P("ens", "model"),
            P(("ens", "fsdp"), "model"),
            P(("ens", "fsdp"), None),
            P("ens", "model"),
            P(("ens", "fsdp", "model")),
            P(("ens", "fsdp", "model")),
        ),
        out_specs=(P(("ens", "model"), None), P(("ens", "model"), None), P("ens")),
        check_vma=False,
    )
```

```python
import functools

import jax
import jax.numpy as jnp
from jax import lax
from jax.experimental import pallas as pl
from jax.experimental.pallas import tpu as pltpu
from jax.sharding import PartitionSpec as P

mix_rate = 2.0
MESH = pl.DeviceIdType.MESH
UP, DOWN = 0, 1
GATE, RISE, NORM = 0, 1, 2
LANES = 128
CUTS = {GATE: (256, 512, 512, 256, 256, 128, 128), RISE: (512, 512, 512, 256, 128, 128), NORM: (1,)}
HOPS = {UP: (4, 3, 4), DOWN: (3, 4, 3)}
ORDER = [(GATE, p) for p in range(len(CUTS[GATE]))] + [(RISE, p) for p in range(len(CUTS[RISE]))]
ORDER.insert(3, (NORM, 0))
ARRIVALS = {
    way: [
        (step, kind, p)
        for step in range(1, 5)
        for kind, p in ORDER
        if step <= HOPS[way][kind]
    ]
    for way in (UP, DOWN)
}
FIRST = (29, 45)
LEAST = min(FIRST)
AHEAD = FIRST.index(LEAST)
MEET = 39


def early(core, way, step, kind, p):
    return ARRIVALS[way].index((step, kind, p)) < FIRST[core]


def shared_early(way, i):
    return i < LEAST


def position(chips):
    f = lax.axis_index("fsdp")
    z, core = f // 2, f % 2
    to = {
        UP: lax.rem(z + 1, chips) * 2 + core,
        DOWN: lax.rem(z + chips - 1, chips) * 2 + core,
    }
    return f, z, core, to, z * 2 + (1 - core)


def owner_of(chips, z, core, way, step):
    back = chips - step if way == UP else step
    return lax.rem(z + back, chips) * 2 + core


def rows_of(kind, p):
    return pl.ds(sum(CUTS[kind][:p]), CUTS[kind][p])


def lanes_of(owner):
    return pl.ds(pl.multiple_of(owner * LANES, LANES), LANES)


def piece_of(held, kind, p, owner):
    if kind == NORM:
        return held[NORM].at[pl.ds(owner, 1)]
    return held[kind].at[rows_of(kind, p), lanes_of(owner)]


def copy_to(source, target, send_sem, recv_sem, fsdp):
    return pltpu.make_async_remote_copy(
        src_ref=source, dst_ref=target, send_sem=send_sem, recv_sem=recv_sem,
        device_id={"fsdp": fsdp}, device_id_type=MESH,
    )


def wait_for(held, kind, rows, sem):
    if rows:
        ref = held[kind].at[pl.ds(0, rows if kind == NORM else rows * LANES // held[kind].shape[1])]
        pltpu.make_async_copy(ref, ref, sem).wait()


def rows_in(pieces):
    return [sum(CUTS[k][p] for k, p in pieces if k == kind) for kind in (GATE, RISE, NORM)]


def each(first, last):
    for i in range(first, last):
        for way in (UP, DOWN):
            if i < len(ARRIVALS[way]):
                yield i, way, *ARRIVALS[way][i]


COUNT = max(len(a) for a in ARRIVALS.values())
MOVED = (GATE, 4)


def moved(way, step, kind, p):
    return (kind, p) == MOVED and way == UP and step == 4


def gather_kernel(
    chips, wg, lg, hg, wu, lu, hu, nt, ns, og, ou, nb,
    wv, lv, hv, ntv, nsv, xb, in_sem, send_sem, recv_sem, sib_sem, x_sem,
):
    loads = []
    for k, (src, dst) in enumerate(
        (
            (lg, lv.at[0]), (hg, hv.at[0]), (wg, wv.at[0]), (nt, ntv), (ns, nsv),
            (lu, lv.at[1]), (hu, hv.at[1]), (wu, wv.at[1]),
        )
    ):
        load = pltpu.make_async_copy(src, dst, in_sem.at[k])
        load.start()
        loads.append(load)

    f, z, core, to, sibling = position(chips)
    m = lax.axis_index("model")
    models = lax.axis_size("model")
    held = (og, ou, nb)
    barrier = pltpu.get_barrier_semaphore()
    for peer in (to[UP], to[DOWN], sibling):
        pl.semaphore_signal(
            barrier, inc=1, device_id={"fsdp": peer}, device_id_type=MESH
        )
    for k in range(1, models):
        pl.semaphore_signal(
            barrier, inc=1, device_id={"model": lax.rem(m + k, models)}, device_id_type=MESH
        )

    def push(kind, p, owner):
        ref = piece_of(held, kind, p, owner)
        copy_to(ref, ref, send_sem.at[2, kind], sib_sem.at[kind], sibling).start()

    def hop(way, step, kind, p, owner):
        ref = piece_of(held, kind, p, owner)
        place = ARRIVALS[way].index((step, kind, p))
        return copy_to(ref, ref, send_sem.at[way, kind], recv_sem.at[way, place], to[way])

    def send_own(kind, p):
        for way in (UP, DOWN):
            hop(way, 1, kind, p, f).start()
        push(kind, p, f)

    def merge(kind, p):
        columns = rows_of(kind, p)
        low_high = lax.dot_general(
            lv[kind], hv[kind, :, columns], (((0,), (0,)), ((), ())),
            preferred_element_type=jnp.float32,
        )
        result = wv[kind, :, columns].astype(jnp.float32) + mix_rate * low_high
        piece_of(held, kind, p, f)[...] = result.T.astype(jnp.bfloat16)

    others = xb.at[pl.ds(0, models - 1)]
    lane = lax.broadcasted_iota(jnp.int32, (1, LANES), 1)
    part = LANES // models

    def norm_part():
        loads[3].wait()
        loads[4].wait()
        xb[m] = jnp.zeros((1, LANES), jnp.float32)
        xb[m, :, pl.ds(0, part)] = (ntv[...] + nsv[...]).reshape(1, part)

    def norm_exchange():
        for k in range(1, models):
            pltpu.make_async_remote_copy(
                src_ref=xb.at[m], dst_ref=xb.at[m], send_sem=x_sem.at[0], recv_sem=x_sem.at[1],
                device_id={"model": lax.rem(m + k, models)}, device_id_type=MESH,
            ).start()

    def norm_row():
        pltpu.make_async_copy(others, others, x_sem.at[1]).wait()
        row = xb[0]
        for k in range(1, models):
            row = jnp.where(lane >= k * part, pltpu.roll(xb[k], k * part, 1), row)
        nb[f] = row

    for k in range(3):
        loads[k].wait()
    merge(GATE, 0)
    merge(GATE, 1)
    pl.semaphore_wait(barrier, 3 + models - 1)
    send_own(GATE, 0)
    norm_part()
    made = [piece for piece in ORDER if piece[0] != NORM]
    pending = [(GATE, 1)]
    for i, piece in enumerate(made[2:]):
        if i == 1:
            norm_exchange()
        if piece == (RISE, 0):
            for k in range(5, 8):
                loads[k].wait()
            norm_row()
            pending.insert(0, (NORM, 0))
        merge(*piece)
        pending.append(piece)
        if piece[0] == GATE and piece[1] < 3:
            if len(pending) > 1:
                send_own(*pending.pop(0))
        elif piece[0] == RISE:
            while len(pending) > 1:
                send_own(*pending.pop(0))
    pltpu.make_async_copy(others, others, x_sem.at[0]).wait()
    while pending:
        send_own(*pending.pop(0))

    def take(c):
        sent = {way: list(ORDER) for way in (UP, DOWN)}
        pushed = list(ORDER)
        for i, way, step, kind, p in each(0, FIRST[c]):
            owner = owner_of(chips, z, core, way, step)
            hop(way, step, kind, p, owner).wait_recv()
            if step < HOPS[way][kind] and early(c, way, step + 1, kind, p):
                hop(way, step + 1, kind, p, owner).start()
                sent[way].append((kind, p))
            if shared_early(way, i):
                push(kind, p, owner)
                pushed.append((kind, p))
        for kind in (NORM, GATE, RISE):
            for way in (UP, DOWN):
                wait_for(held, kind, rows_in(sent[way])[kind], send_sem.at[way, kind])
            wait_for(held, kind, rows_in(pushed)[kind], send_sem.at[2, kind])
            wait_for(held, kind, rows_in(pushed)[kind], sib_sem.at[kind])

    for c in (0, 1):
        pl.when(core == c)(functools.partial(take, c))


def finish_kernel(chips, og, ou, nb, after, lg, lu, ln, send_sem, recv_sem, sib_sem, moved_sem, ready):
    f, z, core, to, sibling = position(chips)
    before, held = (og, ou, nb), (lg, lu, ln)
    barrier = pltpu.get_barrier_semaphore()
    for peer in (to[UP], to[DOWN]):
        pl.semaphore_signal(
            barrier, inc=1, device_id={"fsdp": peer}, device_id_type=MESH
        )

    @pl.when(core == AHEAD)
    def _():
        pl.semaphore_signal(
            barrier, inc=1, device_id={"fsdp": sibling}, device_id_type=MESH
        )
        pl.semaphore_wait(barrier, 2)

    @pl.when(core != AHEAD)
    def _():
        pl.semaphore_wait(barrier, 3)
        pl.semaphore_signal(
            ready, inc=1, device_id={"fsdp": sibling}, device_id_type=MESH
        )

    def push(source, kind, p, owner):
        copy_to(
            piece_of(source, kind, p, owner), piece_of(held, kind, p, owner),
            send_sem.at[2, kind], sib_sem.at[kind], sibling,
        ).start()

    def hop(source, way, step, kind, p, owner):
        place = ARRIVALS[way].index((step, kind, p))
        sem = send_sem.at[3, 0] if moved(way, step, kind, p) else send_sem.at[way, kind]
        return copy_to(
            piece_of(source, kind, p, owner), piece_of(held, kind, p, owner),
            sem, recv_sem.at[way, place], to[way],
        )

    last = chips - 1

    def moved_copy(source, owner):
        return copy_to(
            piece_of(source, *MOVED, owner), piece_of(held, *MOVED, owner),
            moved_sem.at[0], moved_sem.at[1], to[DOWN],
        )

    def forward(source, way, step, kind, p, owner, sent):
        if step < HOPS[way][kind]:
            copy = hop(source, way, step + 1, kind, p, owner)
            if moved(way, step + 1, kind, p):
                pl.when(z != last)(copy.start)
            else:
                copy.start()
                sent[way].append((kind, p))
        elif (kind, p) == MOVED and way == DOWN and step == 3:
            pl.when(z == 1)(moved_copy(source, owner).start)

    def take(c):
        sent = {way: [] for way in (UP, DOWN)}
        pushed, late = [], []
        for i, way, step, kind, p in each(0, FIRST[c]):
            owner = owner_of(chips, z, core, way, step)
            if step == HOPS[way][kind] or not early(c, way, step + 1, kind, p):
                forward(before, way, step, kind, p, owner, sent)
            if not shared_early(way, i):
                late.append((before, kind, p, way, step))

        def push_late():
            while late:
                source, kind, p, way, step = late.pop(0)
                push(source, kind, p, owner_of(chips, z, core, way, step))
                pushed.append((kind, p))

        met = c != AHEAD
        for i, way, step, kind, p in each(FIRST[c], COUNT):
            if not met and i >= MEET:
                pl.semaphore_wait(ready, 1)
                met = True
            if met:
                push_late()
            owner = owner_of(chips, z, core, way, step)
            if moved(way, step, kind, p):
                pl.when(z != 0)(hop(held, way, step, kind, p, owner).wait_recv)
                pl.when(z == 0)(moved_copy(held, owner).wait_recv)
            else:
                hop(held, way, step, kind, p, owner).wait_recv()
            forward(held, way, step, kind, p, owner, sent)
            late.append((held, kind, p, way, step))
        push_late()
        coming = [(kind, p) for _, _, _, kind, p in each(LEAST, COUNT)]
        if all(not early(c, UP, 4, *MOVED) for c in (0, 1)):
            unit = piece_of(held, *MOVED, f)
            kept = pltpu.make_async_copy(unit, unit, send_sem.at[3, 0])
            pl.when(z != last)(kept.wait)
            pl.when(z == 1)(moved_copy(held, f).wait_send)
        for kind in (NORM, GATE, RISE):
            for way in (UP, DOWN):
                wait_for(held, kind, rows_in(sent[way])[kind], send_sem.at[way, kind])
            wait_for(held, kind, rows_in(pushed)[kind], send_sem.at[2, kind])
            wait_for(held, kind, rows_in(coming)[kind], sib_sem.at[kind])

    for c in (0, 1):
        pl.when(core == c)(functools.partial(take, c))


def runs(pieces):
    out = []
    for kind, p in sorted(pieces):
        start, size = sum(CUTS[kind][:p]), CUTS[kind][p]
        if out and out[-1][0] == kind and sum(out[-1][1:]) == start:
            out[-1] = (kind, out[-1][1], out[-1][2] + size)
        else:
            out.append((kind, start, size))
    return out


def store(chips, z, core, c, held, final, sem, sides, own):
    total = [0, 0]
    for mine, (first, last) in ((True, sides[0]), (False, sides[1])):
        line = core if mine else 1 - core
        blocks = {}
        for _, way, step, kind, p in each(first, last):
            if kind != NORM:
                blocks.setdefault((way, step), []).append((kind, p))
        if own:
            blocks[UP, 0] = [piece for piece in ORDER if piece[0] != NORM]
        for (way, step), pieces in blocks.items():
            lanes = lanes_of(owner_of(chips, z, line, way, step))
            for kind, start, size in runs(pieces):
                at = (pl.ds(start, size), lanes)
                pltpu.make_async_copy(held[kind].at[at], final[kind].at[at], sem.at[kind]).start()
                total[kind] += size
    return total


def write_kernel(chips, og, ou, fg, fu, after, sem):
    _, z, core, _, _ = position(chips)
    after[...] = jnp.zeros_like(after)
    held, final = (og, ou), (fg, fu)

    def take(c):
        total = store(chips, z, core, c, held, final, sem, ((0, FIRST[c]), (0, LEAST)), True)
        for kind in (GATE, RISE):
            wait_for(held, kind, total[kind], sem.at[kind])

    for c in (0, 1):
        pl.when(core == c)(functools.partial(take, c))


def write_rest_kernel(chips, fg_in, fu_in, nb, lg, lu, ln, fg, fu, fn, rows, norm, sem):
    f, z, core, _, sibling = position(chips)
    held, final = (lg, lu), (fg, fu)

    def take(c):
        total = store(
            chips, z, core, c, held, final, sem, ((FIRST[c], COUNT), (LEAST, COUNT)), False
        )
        rows[f] = nb[f]
        rows[sibling] = nb[sibling]
        for i, way, step, kind, p in each(0, COUNT):
            if kind == NORM:
                for line, source in ((core, i < FIRST[c]), (1 - core, i < LEAST)):
                    owner = owner_of(chips, z, line, way, step)
                    rows[owner] = nb[owner] if source else ln[owner]
        norm[...] = rows[...].reshape(norm.shape).astype(norm.dtype)
        last = pltpu.make_async_copy(norm, fn, sem.at[2])
        last.start()
        for kind in (GATE, RISE):
            wait_for(held, kind, total[kind], sem.at[kind])
        last.wait()

    for c in (0, 1):
        pl.when(core == c)(functools.partial(take, c))


def solution(mesh):
    fsdp = mesh.shape["fsdp"]
    models = mesh.shape["model"]
    chips = fsdp // 2

    def body(wg, lg, hg, wu, lu, hu, nt, ns):
        depth, width = wg.shape
        rank = lg.shape[1]
        model_width = depth * fsdp
        anywhere = pl.BlockSpec(memory_space=pl.ANY)
        on_chip = pl.BlockSpec(memory_space=pltpu.VMEM)
        final = jax.ShapeDtypeStruct((width, model_width), jnp.bfloat16)
        on_chip_held = (
            pltpu.VMEM((width, model_width), jnp.bfloat16),
            pltpu.VMEM((width, model_width), jnp.bfloat16),
            pltpu.VMEM((fsdp, 1, LANES), jnp.float32),
        )
        ring_sems = [
            pltpu.SemaphoreType.DMA((4, 3)),
            pltpu.SemaphoreType.DMA((2, COUNT)),
            pltpu.SemaphoreType.DMA((3,)),
        ]
        og, ou, nb = pl.pallas_call(
            functools.partial(gather_kernel, chips),
            out_shape=on_chip_held,
            in_specs=[pl.BlockSpec(memory_space=pltpu.HBM)] * 8,
            out_specs=(on_chip,) * 3,
            scratch_shapes=[
                pltpu.VMEM((2, depth, width), jnp.bfloat16),
                pltpu.VMEM((2, rank, depth), jnp.bfloat16),
                pltpu.VMEM((2, rank, width), jnp.bfloat16),
                pltpu.VMEM(nt.shape, jnp.float32),
                pltpu.VMEM(ns.shape, jnp.float32),
                pltpu.VMEM((models, 1, LANES), jnp.float32),
                pltpu.SemaphoreType.DMA((8,)),
                *ring_sems,
                pltpu.SemaphoreType.DMA((2,)),
            ],
            compiler_params=pltpu.CompilerParams(
                collective_id=0, has_side_effects=True, vmem_limit_bytes=50257920
            ),
            name="gather",
        )(wg, lg.T, hg, wu, lu.T, hu, nt, ns)
        fg, fu, after = pl.pallas_call(
            functools.partial(write_kernel, chips),
            out_shape=(final, final, pltpu.VMEM((8, LANES), jnp.float32)),
            in_specs=[on_chip] * 2,
            out_specs=(anywhere, anywhere, on_chip),
            scratch_shapes=[pltpu.SemaphoreType.DMA((2,))],
            compiler_params=pltpu.CompilerParams(vmem_limit_bytes=4 << 20),
            name="write",
        )(og, ou)
        lg2, lu2, ln = pl.pallas_call(
            functools.partial(finish_kernel, chips),
            out_shape=on_chip_held,
            in_specs=[on_chip] * 4,
            out_specs=(on_chip,) * 3,
            scratch_shapes=[
                *ring_sems, pltpu.SemaphoreType.DMA((2,)), pltpu.SemaphoreType.REGULAR
            ],
            compiler_params=pltpu.CompilerParams(
                collective_id=1, has_side_effects=True, vmem_limit_bytes=4 << 20
            ),
            name="finish",
        )(og, ou, nb, after)
        fg, fu, fn = pl.pallas_call(
            functools.partial(write_rest_kernel, chips),
            out_shape=(final, final, jax.ShapeDtypeStruct((fsdp, LANES), jnp.bfloat16)),
            in_specs=[anywhere] * 2 + [on_chip] * 4,
            out_specs=(anywhere,) * 3,
            scratch_shapes=[
                pltpu.VMEM((fsdp, 1, LANES), jnp.float32),
                pltpu.VMEM((fsdp, LANES), jnp.bfloat16),
                pltpu.SemaphoreType.DMA((3,)),
            ],
            input_output_aliases={0: 0, 1: 1},
            compiler_params=pltpu.CompilerParams(vmem_limit_bytes=4 << 20),
            name="write_rest",
        )(fg, fu, nb, lg2, lu2, ln)
        return fg, fu, fn.reshape(fsdp * LANES)

    return jax.shard_map(
        body,
        mesh=mesh,
        in_specs=(
            P(("ens", "fsdp"), "model"),
            P(("ens", "fsdp"), None),
            P("ens", "model"),
            P(("ens", "fsdp"), "model"),
            P(("ens", "fsdp"), None),
            P("ens", "model"),
            P(("ens", "fsdp", "model")),
            P(("ens", "fsdp", "model")),
        ),
        out_specs=(P(("ens", "model"), None), P(("ens", "model"), None), P("ens")),
        check_vma=False,
    )
```

```python
import functools

import jax
import jax.numpy as jnp
from jax import lax
from jax.experimental import pallas as pl
from jax.experimental.pallas import tpu as pltpu
from jax.sharding import PartitionSpec as P

mix_rate = 2.0
MESH = pl.DeviceIdType.MESH
UP, DOWN = 0, 1
GATE, RISE, NORM = 0, 1, 2
LANES = 128
CUTS = {GATE: (256, 512, 512, 128, 384, 128, 128), RISE: (512, 512, 512, 256, 128, 128), NORM: (1,)}
HOPS = {UP: (4, 3, 4), DOWN: (3, 4, 3)}
ORDER = [(GATE, p) for p in range(len(CUTS[GATE]))] + [(RISE, p) for p in range(len(CUTS[RISE]))]
ORDER.insert(len(CUTS[GATE]), (NORM, 0))
ARRIVALS = {
    way: [
        (step, kind, p)
        for step in range(1, 5)
        for kind, p in ORDER
        if step <= HOPS[way][kind]
    ]
    for way in (UP, DOWN)
}
FIRST = (29, 45)
LEAST = min(FIRST)
AHEAD = FIRST.index(LEAST)
MEET = 39


def early(core, way, step, kind, p):
    return ARRIVALS[way].index((step, kind, p)) < FIRST[core]


def shared_early(way, i):
    return i < LEAST


def position(chips):
    f = lax.axis_index("fsdp")
    z, core = f // 2, f % 2
    to = {
        UP: jnp.where(z == chips - 1, 0, z + 1) * 2 + core,
        DOWN: jnp.where(z == 0, chips - 1, z - 1) * 2 + core,
    }
    return f, z, core, to, z * 2 + (1 - core)


def owner_of(chips, z, core, way, step):
    back = chips - step if way == UP else step
    return lax.rem(z + back, chips) * 2 + core


def rows_of(kind, p):
    return pl.ds(sum(CUTS[kind][:p]), CUTS[kind][p])


def lanes_of(owner):
    return pl.ds(pl.multiple_of(owner * LANES, LANES), LANES)


def piece_of(held, kind, p, owner):
    if kind == NORM:
        return held[NORM].at[pl.ds(owner, 1)]
    return held[kind].at[rows_of(kind, p), lanes_of(owner)]


def copy_to(source, target, send_sem, recv_sem, fsdp):
    return pltpu.make_async_remote_copy(
        src_ref=source, dst_ref=target, send_sem=send_sem, recv_sem=recv_sem,
        device_id={"fsdp": fsdp}, device_id_type=MESH,
    )


def wait_for(held, kind, rows, sem):
    if rows:
        ref = held[kind].at[pl.ds(0, rows if kind == NORM else rows * LANES // held[kind].shape[1])]
        pltpu.make_async_copy(ref, ref, sem).wait()


def rows_in(pieces):
    return [sum(CUTS[k][p] for k, p in pieces if k == kind) for kind in (GATE, RISE, NORM)]


def each(first, last):
    for i in range(first, last):
        for way in (UP, DOWN):
            if i < len(ARRIVALS[way]):
                yield i, way, *ARRIVALS[way][i]


COUNT = max(len(a) for a in ARRIVALS.values())
MOVED = (GATE, 4)


def moved(way, step, kind, p):
    return (kind, p) == MOVED and way == UP and step == 4


def gather_kernel(
    chips, wg, lg, hg, wu, lu, hu, nt, ns, og, ou, nb,
    wv, lv, hv, ntv, nsv, xb, in_sem, send_sem, recv_sem, sib_sem, x_sem,
):
    f, z, core, to, sibling = position(chips)
    m = lax.axis_index("model")
    models = lax.axis_size("model")
    held = (og, ou, nb)
    barrier = pltpu.get_barrier_semaphore()
    for peer in (to[UP], to[DOWN], sibling):
        pl.semaphore_signal(
            barrier, inc=1, device_id={"fsdp": peer}, device_id_type=MESH
        )
    right, left = lax.rem(m + 1, models), lax.rem(m + models - 1, models)
    for peer in (right, left):
        pl.semaphore_signal(
            barrier, inc=1, device_id={"model": peer}, device_id_type=MESH
        )

    loads = []
    for k, (src, dst) in enumerate(
        (
            (lg, lv.at[0]), (hg, hv.at[0]), (wg, wv.at[0]), (nt, ntv), (ns, nsv),
            (lu, lv.at[1]), (hu, hv.at[1]), (wu, wv.at[1]),
        )
    ):
        load = pltpu.make_async_copy(src, dst, in_sem.at[k])
        load.start()
        loads.append(load)

    def push(kind, p, owner):
        ref = piece_of(held, kind, p, owner)
        copy_to(ref, ref, send_sem.at[2, kind], sib_sem.at[kind], sibling).start()

    def hop(way, step, kind, p, owner):
        ref = piece_of(held, kind, p, owner)
        place = ARRIVALS[way].index((step, kind, p))
        return copy_to(ref, ref, send_sem.at[way, kind], recv_sem.at[way, place], to[way])

    def send_own(kind, p):
        for way in (UP, DOWN):
            hop(way, 1, kind, p, f).start()
        push(kind, p, f)

    def merge(kind, p):
        columns = rows_of(kind, p)
        low_high = lax.dot_general(
            lv[kind], hv[kind, :, columns], (((0,), (0,)), ((), ())),
            preferred_element_type=jnp.float32,
        )
        result = wv[kind, :, columns].astype(jnp.float32) + mix_rate * low_high
        piece_of(held, kind, p, f)[...] = result.T.astype(jnp.bfloat16)

    others = xb.at[pl.ds(0, models - 1)]
    lane = lax.broadcasted_iota(jnp.int32, (1, LANES), 1)
    part = LANES // models

    def norm_part():
        loads[3].wait()
        loads[4].wait()
        xb[m] = jnp.zeros((1, LANES), jnp.float32)
        xb[m, :, pl.ds(0, part)] = (ntv[...] + nsv[...]).reshape(1, part)

    def norm_send(owner, peer, k):
        pltpu.make_async_remote_copy(
            src_ref=xb.at[owner], dst_ref=xb.at[owner], send_sem=x_sem.at[0], recv_sem=x_sem.at[k],
            device_id={"model": peer}, device_id_type=MESH,
        ).start()

    def norm_arrived(k):
        pltpu.make_async_copy(xb.at[0], xb.at[0], x_sem.at[k]).wait()

    def norm_row():
        row = xb[0]
        for k in range(1, models):
            row = jnp.where(lane >= k * part, pltpu.roll(xb[k], k * part, 1), row)
        nb[f] = row

    for k in range(3):
        loads[k].wait()
    merge(GATE, 0)
    norm_part()
    merge(GATE, 1)
    pl.semaphore_wait(barrier, 5)
    norm_send(m, left, 1)
    norm_send(m, right, 2)
    send_own(GATE, 0)
    merge(GATE, 2)
    send_own(GATE, 1)
    merge(GATE, 3)
    send_own(GATE, 2)
    for p in range(4, len(CUTS[GATE])):
        merge(GATE, p)
        send_own(GATE, p - 1)
    for k in range(5, 8):
        loads[k].wait()
    merge(RISE, 0)
    send_own(GATE, len(CUTS[GATE]) - 1)
    merge(RISE, 1)
    for k in range(2, models - 1):
        norm_arrived(k)
        norm_send(lax.rem(m + models + 1 - k, models), right, k + 1)
    merge(RISE, 2)
    merge(RISE, 3)
    norm_arrived(1)
    norm_arrived(models - 1)
    norm_row()
    for p in range(4, len(CUTS[RISE])):
        merge(RISE, p)
    for piece in ORDER[len(CUTS[GATE]) :]:
        send_own(*piece)
    pltpu.make_async_copy(others, others, x_sem.at[0]).wait()

    def take(c):
        sent = {way: list(ORDER) for way in (UP, DOWN)}
        pushed = list(ORDER)
        for i, way, step, kind, p in each(0, FIRST[c]):
            owner = owner_of(chips, z, core, way, step)
            hop(way, step, kind, p, owner).wait_recv()
            if step < HOPS[way][kind] and early(c, way, step + 1, kind, p):
                hop(way, step + 1, kind, p, owner).start()
                sent[way].append((kind, p))
            if shared_early(way, i):
                push(kind, p, owner)
                pushed.append((kind, p))
        for kind in (NORM, GATE, RISE):
            for way in (UP, DOWN):
                wait_for(held, kind, rows_in(sent[way])[kind], send_sem.at[way, kind])
            wait_for(held, kind, rows_in(pushed)[kind], send_sem.at[2, kind])
            wait_for(held, kind, rows_in(pushed)[kind], sib_sem.at[kind])

    for c in (0, 1):
        pl.when(core == c)(functools.partial(take, c))


def finish_kernel(chips, og, ou, nb, after, lg, lu, ln, send_sem, recv_sem, sib_sem, moved_sem, ready):
    f, z, core, to, sibling = position(chips)
    before, held = (og, ou, nb), (lg, lu, ln)
    barrier = pltpu.get_barrier_semaphore()
    for peer in (to[UP], to[DOWN]):
        pl.semaphore_signal(
            barrier, inc=1, device_id={"fsdp": peer}, device_id_type=MESH
        )

    @pl.when(core == AHEAD)
    def _():
        pl.semaphore_signal(
            barrier, inc=1, device_id={"fsdp": sibling}, device_id_type=MESH
        )
        pl.semaphore_wait(barrier, 2)

    @pl.when(core != AHEAD)
    def _():
        pl.semaphore_wait(barrier, 3)
        pl.semaphore_signal(
            ready, inc=1, device_id={"fsdp": sibling}, device_id_type=MESH
        )

    def push(source, kind, p, owner):
        copy_to(
            piece_of(source, kind, p, owner), piece_of(held, kind, p, owner),
            send_sem.at[2, kind], sib_sem.at[kind], sibling,
        ).start()

    def hop(source, way, step, kind, p, owner):
        place = ARRIVALS[way].index((step, kind, p))
        sem = send_sem.at[3, 0] if moved(way, step, kind, p) else send_sem.at[way, kind]
        return copy_to(
            piece_of(source, kind, p, owner), piece_of(held, kind, p, owner),
            sem, recv_sem.at[way, place], to[way],
        )

    last = chips - 1

    def moved_copy(source, owner):
        return copy_to(
            piece_of(source, *MOVED, owner), piece_of(held, *MOVED, owner),
            moved_sem.at[0], moved_sem.at[1], to[DOWN],
        )

    def forward(source, way, step, kind, p, owner, sent):
        if step < HOPS[way][kind]:
            copy = hop(source, way, step + 1, kind, p, owner)
            if moved(way, step + 1, kind, p):
                pl.when(z != last)(copy.start)
            else:
                copy.start()
                sent[way].append((kind, p))
        elif (kind, p) == MOVED and way == DOWN and step == 3:
            pl.when(z == 1)(moved_copy(source, owner).start)

    def take(c):
        sent = {way: [] for way in (UP, DOWN)}
        pushed, late = [], []
        for i, way, step, kind, p in each(0, FIRST[c]):
            owner = owner_of(chips, z, core, way, step)
            if step == HOPS[way][kind] or not early(c, way, step + 1, kind, p):
                forward(before, way, step, kind, p, owner, sent)
            if not shared_early(way, i):
                late.append((before, kind, p, way, step))

        def push_late():
            while late:
                source, kind, p, way, step = late.pop(0)
                push(source, kind, p, owner_of(chips, z, core, way, step))
                pushed.append((kind, p))

        met = c != AHEAD
        for i, way, step, kind, p in each(FIRST[c], COUNT):
            if not met and i >= MEET:
                pl.semaphore_wait(ready, 1)
                met = True
            if met:
                push_late()
            owner = owner_of(chips, z, core, way, step)
            if moved(way, step, kind, p):
                pl.when(z != 0)(hop(held, way, step, kind, p, owner).wait_recv)
                pl.when(z == 0)(moved_copy(held, owner).wait_recv)
            else:
                hop(held, way, step, kind, p, owner).wait_recv()
            forward(held, way, step, kind, p, owner, sent)
            late.append((held, kind, p, way, step))
        push_late()
        coming = [(kind, p) for _, _, _, kind, p in each(LEAST, COUNT)]
        if all(not early(c, UP, 4, *MOVED) for c in (0, 1)):
            unit = piece_of(held, *MOVED, f)
            kept = pltpu.make_async_copy(unit, unit, send_sem.at[3, 0])
            pl.when(z != last)(kept.wait)
            pl.when(z == 1)(moved_copy(held, f).wait_send)
        for kind in (NORM, GATE, RISE):
            for way in (UP, DOWN):
                wait_for(held, kind, rows_in(sent[way])[kind], send_sem.at[way, kind])
            wait_for(held, kind, rows_in(pushed)[kind], send_sem.at[2, kind])
            wait_for(held, kind, rows_in(coming)[kind], sib_sem.at[kind])

    for c in (0, 1):
        pl.when(core == c)(functools.partial(take, c))


def runs(pieces):
    out = []
    for kind, p in sorted(pieces):
        start, size = sum(CUTS[kind][:p]), CUTS[kind][p]
        if out and out[-1][0] == kind and sum(out[-1][1:]) == start:
            out[-1] = (kind, out[-1][1], out[-1][2] + size)
        else:
            out.append((kind, start, size))
    return out


def store(chips, z, core, c, held, final, sem, sides, own):
    total = [0, 0]
    for mine, (first, last) in ((False, sides[1]), (True, sides[0])):
        line = core if mine else 1 - core
        blocks = {}
        for _, way, step, kind, p in each(first, last):
            if kind != NORM:
                blocks.setdefault((way, step), []).append((kind, p))
        if own:
            blocks[UP, 0] = [piece for piece in ORDER if piece[0] != NORM]
        for (way, step), pieces in blocks.items():
            lanes = lanes_of(owner_of(chips, z, line, way, step))
            for kind, start, size in runs(pieces):
                at = (pl.ds(start, size), lanes)
                pltpu.make_async_copy(held[kind].at[at], final[kind].at[at], sem.at[kind]).start()
                total[kind] += size
    return total


def write_kernel(chips, og, ou, fg, fu, after, sem):
    _, z, core, _, _ = position(chips)
    after[...] = jnp.zeros_like(after)
    held, final = (og, ou), (fg, fu)

    def take(c):
        total = store(chips, z, core, c, held, final, sem, ((0, FIRST[c]), (0, LEAST)), True)
        for kind in (GATE, RISE):
            wait_for(held, kind, total[kind], sem.at[kind])

    for c in (0, 1):
        pl.when(core == c)(functools.partial(take, c))


def write_rest_kernel(chips, fg_in, fu_in, nb, lg, lu, ln, fg, fu, fn, rows, norm, sem):
    f, z, core, _, sibling = position(chips)
    held, final = (lg, lu), (fg, fu)

    def take(c):
        total = store(
            chips, z, core, c, held, final, sem, ((FIRST[c], COUNT), (LEAST, COUNT)), False
        )
        rows[f] = nb[f]
        rows[sibling] = nb[sibling]
        for i, way, step, kind, p in each(0, COUNT):
            if kind == NORM:
                for line, source in ((core, i < FIRST[c]), (1 - core, i < LEAST)):
                    owner = owner_of(chips, z, line, way, step)
                    rows[owner] = nb[owner] if source else ln[owner]
        norm[...] = rows[...].reshape(norm.shape).astype(norm.dtype)
        last = pltpu.make_async_copy(norm, fn, sem.at[2])
        last.start()
        for kind in (GATE, RISE):
            wait_for(held, kind, total[kind], sem.at[kind])
        last.wait()

    for c in (0, 1):
        pl.when(core == c)(functools.partial(take, c))


def solution(mesh):
    fsdp = mesh.shape["fsdp"]
    models = mesh.shape["model"]
    chips = fsdp // 2

    def body(wg, lg, hg, wu, lu, hu, nt, ns):
        depth, width = wg.shape
        rank = lg.shape[1]
        model_width = depth * fsdp
        anywhere = pl.BlockSpec(memory_space=pl.ANY)
        on_chip = pl.BlockSpec(memory_space=pltpu.VMEM)
        final = jax.ShapeDtypeStruct((width, model_width), jnp.bfloat16)
        on_chip_held = (
            pltpu.VMEM((width, model_width), jnp.bfloat16),
            pltpu.VMEM((width, model_width), jnp.bfloat16),
            pltpu.VMEM((fsdp, 1, LANES), jnp.float32),
        )
        ring_sems = [
            pltpu.SemaphoreType.DMA((4, 3)),
            pltpu.SemaphoreType.DMA((2, COUNT)),
            pltpu.SemaphoreType.DMA((3,)),
        ]
        og, ou, nb = pl.pallas_call(
            functools.partial(gather_kernel, chips),
            out_shape=on_chip_held,
            in_specs=[pl.BlockSpec(memory_space=pltpu.HBM)] * 8,
            out_specs=(on_chip,) * 3,
            scratch_shapes=[
                pltpu.VMEM((2, depth, width), jnp.bfloat16),
                pltpu.VMEM((2, rank, depth), jnp.bfloat16),
                pltpu.VMEM((2, rank, width), jnp.bfloat16),
                pltpu.VMEM(nt.shape, jnp.float32),
                pltpu.VMEM(ns.shape, jnp.float32),
                pltpu.VMEM((models, 1, LANES), jnp.float32),
                pltpu.SemaphoreType.DMA((8,)),
                *ring_sems,
                pltpu.SemaphoreType.DMA((models,)),
            ],
            compiler_params=pltpu.CompilerParams(
                collective_id=0, has_side_effects=True, vmem_limit_bytes=50257920
            ),
            name="gather",
        )(wg, lg.T, hg, wu, lu.T, hu, nt, ns)
        fg, fu, after = pl.pallas_call(
            functools.partial(write_kernel, chips),
            out_shape=(final, final, pltpu.VMEM((8, LANES), jnp.float32)),
            in_specs=[on_chip] * 2,
            out_specs=(anywhere, anywhere, on_chip),
            scratch_shapes=[pltpu.SemaphoreType.DMA((2,))],
            compiler_params=pltpu.CompilerParams(vmem_limit_bytes=4 << 20),
            name="write",
        )(og, ou)
        lg2, lu2, ln = pl.pallas_call(
            functools.partial(finish_kernel, chips),
            out_shape=on_chip_held,
            in_specs=[on_chip] * 4,
            out_specs=(on_chip,) * 3,
            scratch_shapes=[
                *ring_sems, pltpu.SemaphoreType.DMA((2,)), pltpu.SemaphoreType.REGULAR
            ],
            compiler_params=pltpu.CompilerParams(
                collective_id=1, has_side_effects=True, vmem_limit_bytes=4 << 20
            ),
            name="finish",
        )(og, ou, nb, after)
        fg, fu, fn = pl.pallas_call(
            functools.partial(write_rest_kernel, chips),
            out_shape=(final, final, jax.ShapeDtypeStruct((fsdp, LANES), jnp.bfloat16)),
            in_specs=[anywhere] * 2 + [on_chip] * 4,
            out_specs=(anywhere,) * 3,
            scratch_shapes=[
                pltpu.VMEM((fsdp, 1, LANES), jnp.float32),
                pltpu.VMEM((fsdp, LANES), jnp.bfloat16),
                pltpu.SemaphoreType.DMA((3,)),
            ],
            input_output_aliases={0: 0, 1: 1},
            compiler_params=pltpu.CompilerParams(vmem_limit_bytes=4 << 20),
            name="write_rest",
        )(fg, fu, nb, lg2, lu2, ln)
        return fg, fu, fn.reshape(fsdp * LANES)

    return jax.shard_map(
        body,
        mesh=mesh,
        in_specs=(
            P(("ens", "fsdp"), "model"),
            P(("ens", "fsdp"), None),
            P("ens", "model"),
            P(("ens", "fsdp"), "model"),
            P(("ens", "fsdp"), None),
            P("ens", "model"),
            P(("ens", "fsdp", "model")),
            P(("ens", "fsdp", "model")),
        ),
        out_specs=(P(("ens", "model"), None), P(("ens", "model"), None), P("ens")),
        check_vma=False,
    )
```

```python
import functools
import itertools

import jax
import jax.numpy as jnp
from jax import lax
from jax.experimental import pallas as pl
from jax.experimental.pallas import tpu as pltpu
from jax.sharding import PartitionSpec as P

mix_rate = 2.0
MESH = pl.DeviceIdType.MESH
UP, DOWN = 0, 1
GATE, RISE, NORM = 0, 1, 2
LANES = 128
CUTS = {GATE: (256, 512, 512, 128, 384, 128, 128), RISE: (512, 512, 512, 256, 128, 128), NORM: (1,)}
HOPS = {UP: (4, 3, 4), DOWN: (3, 4, 3)}
BLOCK = {kind: [(kind, p) for p in range(len(CUTS[kind]))] for kind in (GATE, RISE, NORM)}
ORDERS = {
    UP: BLOCK[GATE] + BLOCK[NORM] + BLOCK[RISE],
    DOWN: BLOCK[RISE] + BLOCK[NORM] + BLOCK[GATE],
}
ORDER = ORDERS[UP]
ARRIVALS = {
    way: [
        (step, kind, p)
        for step in range(1, 5)
        for kind, p in ORDERS[way]
        if step <= HOPS[way][kind]
    ]
    for way in (UP, DOWN)
}
FIRST = (29, 45)
LEAST = min(FIRST)
AHEAD = FIRST.index(LEAST)
MEET = 41


def early(core, way, step, kind, p):
    return ARRIVALS[way].index((step, kind, p)) < FIRST[core]


def shared_early(way, i):
    return i < LEAST


def position(chips):
    f = lax.axis_index("fsdp")
    z, core = f // 2, f % 2
    to = {
        UP: jnp.where(z == chips - 1, 0, z + 1) * 2 + core,
        DOWN: jnp.where(z == 0, chips - 1, z - 1) * 2 + core,
    }
    return f, z, core, to, z * 2 + (1 - core)


def owner_of(chips, z, core, way, step):
    back = chips - step if way == UP else step
    return lax.rem(z + back, chips) * 2 + core


def rows_of(kind, p):
    return pl.ds(sum(CUTS[kind][:p]), CUTS[kind][p])


def lanes_of(owner):
    return pl.ds(pl.multiple_of(owner * LANES, LANES), LANES)


def piece_of(held, kind, p, owner):
    if kind == NORM:
        return held[NORM].at[pl.ds(owner, 1)]
    return held[kind].at[rows_of(kind, p), lanes_of(owner)]


def copy_to(source, target, send_sem, recv_sem, fsdp):
    return pltpu.make_async_remote_copy(
        src_ref=source, dst_ref=target, send_sem=send_sem, recv_sem=recv_sem,
        device_id={"fsdp": fsdp}, device_id_type=MESH,
    )


def wait_for(held, kind, rows, sem):
    if rows:
        ref = held[kind].at[pl.ds(0, rows if kind == NORM else rows * LANES // held[kind].shape[1])]
        pltpu.make_async_copy(ref, ref, sem).wait()


def rows_in(pieces):
    return [sum(CUTS[k][p] for k, p in pieces if k == kind) for kind in (GATE, RISE, NORM)]


def each(first, last):
    for i in range(first, last):
        for way in (UP, DOWN):
            if i < len(ARRIVALS[way]):
                yield i, way, *ARRIVALS[way][i]


COUNT = max(len(a) for a in ARRIVALS.values())
MOVED = (GATE, 4)


def moved(way, step, kind, p):
    return (kind, p) == MOVED and way == UP and step == 4


def gather_kernel(
    chips, wg, lg, hg, wu, lu, hu, nt, ns, og, ou, nb,
    wv, lv, hv, ntv, nsv, xb, in_sem, send_sem, recv_sem, sib_sem, x_sem,
):
    f, z, core, to, sibling = position(chips)
    m = lax.axis_index("model")
    models = lax.axis_size("model")
    held = (og, ou, nb)
    barrier = pltpu.get_barrier_semaphore()
    for peer in (to[UP], to[DOWN], sibling):
        pl.semaphore_signal(
            barrier, inc=1, device_id={"fsdp": peer}, device_id_type=MESH
        )
    right, left = lax.rem(m + 1, models), lax.rem(m + models - 1, models)
    for peer in (right, left):
        pl.semaphore_signal(
            barrier, inc=1, device_id={"model": peer}, device_id_type=MESH
        )

    loads = []
    for k, (src, dst) in enumerate(
        (
            (lg, lv.at[0]), (hg, hv.at[0]), (wg, wv.at[0]), (nt, ntv), (ns, nsv),
            (lu, lv.at[1]), (hu, hv.at[1]), (wu, wv.at[1]),
        )
    ):
        load = pltpu.make_async_copy(src, dst, in_sem.at[k])
        load.start()
        loads.append(load)

    def push(kind, p, owner):
        ref = piece_of(held, kind, p, owner)
        copy_to(ref, ref, send_sem.at[2, kind], sib_sem.at[kind], sibling).start()

    def hop(way, step, kind, p, owner):
        ref = piece_of(held, kind, p, owner)
        place = ARRIVALS[way].index((step, kind, p))
        return copy_to(ref, ref, send_sem.at[way, kind], recv_sem.at[way, place], to[way])

    def send_own(way, kind, p):
        hop(way, 1, kind, p, f).start()

    def merge(kind, p):
        columns = rows_of(kind, p)
        low_high = lax.dot_general(
            lv[kind], hv[kind, :, columns], (((0,), (0,)), ((), ())),
            preferred_element_type=jnp.float32,
        )
        result = wv[kind, :, columns].astype(jnp.float32) + mix_rate * low_high
        piece_of(held, kind, p, f)[...] = result.T.astype(jnp.bfloat16)

    others = xb.at[pl.ds(0, models - 1)]
    lane = lax.broadcasted_iota(jnp.int32, (1, LANES), 1)
    part = LANES // models

    def norm_part():
        loads[3].wait()
        loads[4].wait()
        xb[m] = jnp.zeros((1, LANES), jnp.float32)
        xb[m, :, pl.ds(0, part)] = (ntv[...] + nsv[...]).reshape(1, part)

    def norm_send(owner, peer, k):
        pltpu.make_async_remote_copy(
            src_ref=xb.at[owner], dst_ref=xb.at[owner], send_sem=x_sem.at[0], recv_sem=x_sem.at[k],
            device_id={"model": peer}, device_id_type=MESH,
        ).start()

    def norm_arrived(k):
        pltpu.make_async_copy(xb.at[0], xb.at[0], x_sem.at[k]).wait()

    def norm_row():
        row = xb[0]
        for k in range(1, models):
            row = jnp.where(lane >= k * part, pltpu.roll(xb[k], k * part, 1), row)
        nb[f] = row

    made = [
        piece
        for pair in itertools.zip_longest(BLOCK[GATE], BLOCK[RISE])
        for piece in pair
        if piece
    ]

    def first_send(kind, p):
        send_own(UP if kind == GATE else DOWN, kind, p)
        push(kind, p, f)

    for k in (0, 1, 2):
        loads[k].wait()
    merge(*made[0])
    norm_part()
    for k in (5, 6, 7):
        loads[k].wait()
    merge(*made[1])
    merge(*made[2])
    pl.semaphore_wait(barrier, 5)
    norm_send(m, left, 1)
    norm_send(m, right, 2)
    first_send(*made[0])
    first_send(*made[1])
    for before, piece in zip(made[2:], made[3:]):
        merge(*piece)
        first_send(*before)
    for k in range(2, models - 1):
        norm_arrived(k)
        norm_send(lax.rem(m + models + 1 - k, models), right, k + 1)
    first_send(*made[-1])
    norm_arrived(1)
    norm_arrived(models - 1)
    norm_row()
    for way, kind in ((UP, RISE), (DOWN, GATE)):
        send_own(way, *BLOCK[kind][0])
        if way == UP:
            push(NORM, 0, f)
        send_own(way, NORM, 0)
        for piece in BLOCK[kind][1:]:
            send_own(way, *piece)
    pltpu.make_async_copy(others, others, x_sem.at[0]).wait()

    def take(c):
        sent = {way: list(ORDER) for way in (UP, DOWN)}
        pushed = list(ORDER)
        for i, way, step, kind, p in each(0, FIRST[c]):
            owner = owner_of(chips, z, core, way, step)
            hop(way, step, kind, p, owner).wait_recv()
            if step < HOPS[way][kind] and early(c, way, step + 1, kind, p):
                hop(way, step + 1, kind, p, owner).start()
                sent[way].append((kind, p))
            if shared_early(way, i):
                push(kind, p, owner)
                pushed.append((kind, p))
        for kind in (NORM, GATE, RISE):
            for way in (UP, DOWN):
                wait_for(held, kind, rows_in(sent[way])[kind], send_sem.at[way, kind])
            wait_for(held, kind, rows_in(pushed)[kind], send_sem.at[2, kind])
            wait_for(held, kind, rows_in(pushed)[kind], sib_sem.at[kind])

    for c in (0, 1):
        pl.when(core == c)(functools.partial(take, c))


def finish_kernel(chips, og, ou, nb, after, lg, lu, ln, send_sem, recv_sem, sib_sem, moved_sem, ready):
    f, z, core, to, sibling = position(chips)
    before, held = (og, ou, nb), (lg, lu, ln)
    barrier = pltpu.get_barrier_semaphore()
    for peer in (to[UP], to[DOWN]):
        pl.semaphore_signal(
            barrier, inc=1, device_id={"fsdp": peer}, device_id_type=MESH
        )

    @pl.when(core == AHEAD)
    def _():
        pl.semaphore_signal(
            barrier, inc=1, device_id={"fsdp": sibling}, device_id_type=MESH
        )
        pl.semaphore_wait(barrier, 2)

    @pl.when(core != AHEAD)
    def _():
        pl.semaphore_wait(barrier, 3)
        pl.semaphore_signal(
            ready, inc=1, device_id={"fsdp": sibling}, device_id_type=MESH
        )

    def push(source, kind, p, owner):
        copy_to(
            piece_of(source, kind, p, owner), piece_of(held, kind, p, owner),
            send_sem.at[2, kind], sib_sem.at[kind], sibling,
        ).start()

    def hop(source, way, step, kind, p, owner):
        place = ARRIVALS[way].index((step, kind, p))
        sem = send_sem.at[3, 0] if moved(way, step, kind, p) else send_sem.at[way, kind]
        return copy_to(
            piece_of(source, kind, p, owner), piece_of(held, kind, p, owner),
            sem, recv_sem.at[way, place], to[way],
        )

    last = chips - 1

    def moved_copy(source, owner):
        return copy_to(
            piece_of(source, *MOVED, owner), piece_of(held, *MOVED, owner),
            moved_sem.at[0], moved_sem.at[1], to[DOWN],
        )

    def forward(source, way, step, kind, p, owner, sent):
        if step < HOPS[way][kind]:
            copy = hop(source, way, step + 1, kind, p, owner)
            if moved(way, step + 1, kind, p):
                pl.when(z != last)(copy.start)
            else:
                copy.start()
                sent[way].append((kind, p))
        elif (kind, p) == MOVED and way == DOWN and step == 3:
            pl.when(z == 1)(moved_copy(source, owner).start)

    def take(c):
        sent = {way: [] for way in (UP, DOWN)}
        pushed, late = [], []
        for i, way, step, kind, p in each(0, FIRST[c]):
            owner = owner_of(chips, z, core, way, step)
            if step == HOPS[way][kind] or not early(c, way, step + 1, kind, p):
                forward(before, way, step, kind, p, owner, sent)
            if not shared_early(way, i):
                late.append((before, kind, p, way, step))

        def push_late():
            while late:
                source, kind, p, way, step = late.pop(0)
                push(source, kind, p, owner_of(chips, z, core, way, step))
                pushed.append((kind, p))

        met = c != AHEAD
        for i, way, step, kind, p in each(FIRST[c], COUNT):
            if not met and i >= MEET:
                pl.semaphore_wait(ready, 1)
                met = True
            if met:
                push_late()
            owner = owner_of(chips, z, core, way, step)
            if moved(way, step, kind, p):
                pl.when(z != 0)(hop(held, way, step, kind, p, owner).wait_recv)
                pl.when(z == 0)(moved_copy(held, owner).wait_recv)
            else:
                hop(held, way, step, kind, p, owner).wait_recv()
            forward(held, way, step, kind, p, owner, sent)
            late.append((held, kind, p, way, step))
        push_late()
        coming = [(kind, p) for _, _, _, kind, p in each(LEAST, COUNT)]
        if all(not early(c, UP, 4, *MOVED) for c in (0, 1)):
            unit = piece_of(held, *MOVED, f)
            kept = pltpu.make_async_copy(unit, unit, send_sem.at[3, 0])
            pl.when(z != last)(kept.wait)
            pl.when(z == 1)(moved_copy(held, f).wait_send)
        for kind in (NORM, GATE, RISE):
            for way in (UP, DOWN):
                wait_for(held, kind, rows_in(sent[way])[kind], send_sem.at[way, kind])
            wait_for(held, kind, rows_in(pushed)[kind], send_sem.at[2, kind])
            wait_for(held, kind, rows_in(coming)[kind], sib_sem.at[kind])

    for c in (0, 1):
        pl.when(core == c)(functools.partial(take, c))


def runs(pieces):
    out = []
    for kind, p in sorted(pieces):
        start, size = sum(CUTS[kind][:p]), CUTS[kind][p]
        if out and out[-1][0] == kind and sum(out[-1][1:]) == start:
            out[-1] = (kind, out[-1][1], out[-1][2] + size)
        else:
            out.append((kind, start, size))
    return out


def store(chips, z, core, c, held, final, sem, sides, own):
    total = [0, 0]
    for mine, (first, last) in ((False, sides[1]), (True, sides[0])):
        line = core if mine else 1 - core
        blocks = {}
        for _, way, step, kind, p in each(first, last):
            if kind != NORM:
                blocks.setdefault((way, step), []).append((kind, p))
        if own:
            blocks[UP, 0] = [piece for piece in ORDER if piece[0] != NORM]
        for (way, step), pieces in blocks.items():
            lanes = lanes_of(owner_of(chips, z, line, way, step))
            for kind, start, size in runs(pieces):
                at = (pl.ds(start, size), lanes)
                pltpu.make_async_copy(held[kind].at[at], final[kind].at[at], sem.at[kind]).start()
                total[kind] += size
    return total


def write_kernel(chips, og, ou, fg, fu, after, sem):
    _, z, core, _, _ = position(chips)
    after[...] = jnp.zeros_like(after)
    held, final = (og, ou), (fg, fu)

    def take(c):
        total = store(chips, z, core, c, held, final, sem, ((0, FIRST[c]), (0, LEAST)), True)
        for kind in (GATE, RISE):
            wait_for(held, kind, total[kind], sem.at[kind])

    for c in (0, 1):
        pl.when(core == c)(functools.partial(take, c))


def write_rest_kernel(chips, fg_in, fu_in, nb, lg, lu, ln, fg, fu, fn, rows, norm, sem):
    f, z, core, _, sibling = position(chips)
    held, final = (lg, lu), (fg, fu)

    def take(c):
        total = store(
            chips, z, core, c, held, final, sem, ((FIRST[c], COUNT), (LEAST, COUNT)), False
        )
        rows[f] = nb[f]
        rows[sibling] = nb[sibling]
        for i, way, step, kind, p in each(0, COUNT):
            if kind == NORM:
                for line, source in ((core, i < FIRST[c]), (1 - core, i < LEAST)):
                    owner = owner_of(chips, z, line, way, step)
                    rows[owner] = nb[owner] if source else ln[owner]
        norm[...] = rows[...].reshape(norm.shape).astype(norm.dtype)
        last = pltpu.make_async_copy(norm, fn, sem.at[2])
        last.start()
        for kind in (GATE, RISE):
            wait_for(held, kind, total[kind], sem.at[kind])
        last.wait()

    for c in (0, 1):
        pl.when(core == c)(functools.partial(take, c))


def solution(mesh):
    fsdp = mesh.shape["fsdp"]
    models = mesh.shape["model"]
    chips = fsdp // 2

    def body(wg, lg, hg, wu, lu, hu, nt, ns):
        depth, width = wg.shape
        rank = lg.shape[1]
        model_width = depth * fsdp
        anywhere = pl.BlockSpec(memory_space=pl.ANY)
        on_chip = pl.BlockSpec(memory_space=pltpu.VMEM)
        final = jax.ShapeDtypeStruct((width, model_width), jnp.bfloat16)
        on_chip_held = (
            pltpu.VMEM((width, model_width), jnp.bfloat16),
            pltpu.VMEM((width, model_width), jnp.bfloat16),
            pltpu.VMEM((fsdp, 1, LANES), jnp.float32),
        )
        ring_sems = [
            pltpu.SemaphoreType.DMA((4, 3)),
            pltpu.SemaphoreType.DMA((2, COUNT)),
            pltpu.SemaphoreType.DMA((3,)),
        ]
        og, ou, nb = pl.pallas_call(
            functools.partial(gather_kernel, chips),
            out_shape=on_chip_held,
            in_specs=[pl.BlockSpec(memory_space=pltpu.HBM)] * 8,
            out_specs=(on_chip,) * 3,
            scratch_shapes=[
                pltpu.VMEM((2, depth, width), jnp.bfloat16),
                pltpu.VMEM((2, rank, depth), jnp.bfloat16),
                pltpu.VMEM((2, rank, width), jnp.bfloat16),
                pltpu.VMEM(nt.shape, jnp.float32),
                pltpu.VMEM(ns.shape, jnp.float32),
                pltpu.VMEM((models, 1, LANES), jnp.float32),
                pltpu.SemaphoreType.DMA((8,)),
                *ring_sems,
                pltpu.SemaphoreType.DMA((models,)),
            ],
            compiler_params=pltpu.CompilerParams(
                collective_id=0, has_side_effects=True, vmem_limit_bytes=50257920
            ),
            name="gather",
        )(wg, lg.T, hg, wu, lu.T, hu, nt, ns)
        fg, fu, after = pl.pallas_call(
            functools.partial(write_kernel, chips),
            out_shape=(final, final, pltpu.VMEM((8, LANES), jnp.float32)),
            in_specs=[on_chip] * 2,
            out_specs=(anywhere, anywhere, on_chip),
            scratch_shapes=[pltpu.SemaphoreType.DMA((2,))],
            compiler_params=pltpu.CompilerParams(vmem_limit_bytes=4 << 20),
            name="write",
        )(og, ou)
        lg2, lu2, ln = pl.pallas_call(
            functools.partial(finish_kernel, chips),
            out_shape=on_chip_held,
            in_specs=[on_chip] * 4,
            out_specs=(on_chip,) * 3,
            scratch_shapes=[
                *ring_sems, pltpu.SemaphoreType.DMA((2,)), pltpu.SemaphoreType.REGULAR
            ],
            compiler_params=pltpu.CompilerParams(
                collective_id=1, has_side_effects=True, vmem_limit_bytes=4 << 20
            ),
            name="finish",
        )(og, ou, nb, after)
        fg, fu, fn = pl.pallas_call(
            functools.partial(write_rest_kernel, chips),
            out_shape=(final, final, jax.ShapeDtypeStruct((fsdp, LANES), jnp.bfloat16)),
            in_specs=[anywhere] * 2 + [on_chip] * 4,
            out_specs=(anywhere,) * 3,
            scratch_shapes=[
                pltpu.VMEM((fsdp, 1, LANES), jnp.float32),
                pltpu.VMEM((fsdp, LANES), jnp.bfloat16),
                pltpu.SemaphoreType.DMA((3,)),
            ],
            input_output_aliases={0: 0, 1: 1},
            compiler_params=pltpu.CompilerParams(vmem_limit_bytes=4 << 20),
            name="write_rest",
        )(fg, fu, nb, lg2, lu2, ln)
        return fg, fu, fn.reshape(fsdp * LANES)

    return jax.shard_map(
        body,
        mesh=mesh,
        in_specs=(
            P(("ens", "fsdp"), "model"),
            P(("ens", "fsdp"), None),
            P("ens", "model"),
            P(("ens", "fsdp"), "model"),
            P(("ens", "fsdp"), None),
            P("ens", "model"),
            P(("ens", "fsdp", "model")),
            P(("ens", "fsdp", "model")),
        ),
        out_specs=(P(("ens", "model"), None), P(("ens", "model"), None), P("ens")),
        check_vma=False,
    )
```

```python
import functools
import itertools

import jax
import jax.numpy as jnp
from jax import lax
from jax.experimental import pallas as pl
from jax.experimental.pallas import tpu as pltpu
from jax.sharding import PartitionSpec as P

mix_rate = 2.0
MESH = pl.DeviceIdType.MESH
UP, DOWN = 0, 1
GATE, RISE, NORM = 0, 1, 2
LANES = 128
CUTS = {GATE: (256, 512, 512, 128, 384, 128, 128), RISE: (512, 512, 512, 256, 128, 128), NORM: (1,)}
HOPS = {UP: (4, 3, 4), DOWN: (3, 4, 3)}
BLOCK = {kind: [(kind, p) for p in range(len(CUTS[kind]))] for kind in (GATE, RISE, NORM)}
ORDERS = {
    UP: BLOCK[GATE] + BLOCK[NORM] + BLOCK[RISE],
    DOWN: BLOCK[RISE] + BLOCK[NORM] + BLOCK[GATE],
}
ORDER = ORDERS[UP]
ARRIVALS = {
    way: [
        (step, kind, p)
        for step in range(1, 5)
        for kind, p in ORDERS[way]
        if step <= HOPS[way][kind]
    ]
    for way in (UP, DOWN)
}
FIRST = (29, 46)
LEAST = min(FIRST)
AHEAD = FIRST.index(LEAST)
MEET = 41


def early(core, way, step, kind, p):
    return ARRIVALS[way].index((step, kind, p)) < FIRST[core]


def shared_early(way, i):
    return i < LEAST


def position(chips):
    f = lax.axis_index("fsdp")
    z, core = f // 2, f % 2
    to = {
        UP: jnp.where(z == chips - 1, 0, z + 1) * 2 + core,
        DOWN: jnp.where(z == 0, chips - 1, z - 1) * 2 + core,
    }
    return f, z, core, to, z * 2 + (1 - core)


def owner_of(chips, z, core, way, step):
    back = chips - step if way == UP else step
    return lax.rem(z + back, chips) * 2 + core


def rows_of(kind, p):
    return pl.ds(sum(CUTS[kind][:p]), CUTS[kind][p])


def lanes_of(owner):
    return pl.ds(pl.multiple_of(owner * LANES, LANES), LANES)


def piece_of(held, kind, p, owner):
    if kind == NORM:
        return held[NORM].at[pl.ds(owner, 1)]
    return held[kind].at[rows_of(kind, p), lanes_of(owner)]


def copy_to(source, target, send_sem, recv_sem, fsdp):
    return pltpu.make_async_remote_copy(
        src_ref=source, dst_ref=target, send_sem=send_sem, recv_sem=recv_sem,
        device_id={"fsdp": fsdp}, device_id_type=MESH,
    )


def wait_for(held, kind, rows, sem):
    if rows:
        ref = held[kind].at[pl.ds(0, rows if kind == NORM else rows * LANES // held[kind].shape[1])]
        pltpu.make_async_copy(ref, ref, sem).wait()


def rows_in(pieces):
    return [sum(CUTS[k][p] for k, p in pieces if k == kind) for kind in (GATE, RISE, NORM)]


def each(first, last):
    for i in range(first, last):
        for way in (UP, DOWN):
            if i < len(ARRIVALS[way]):
                yield i, way, *ARRIVALS[way][i]


COUNT = max(len(a) for a in ARRIVALS.values())
MOVED = (GATE, 4)


def moved(way, step, kind, p):
    return (kind, p) == MOVED and way == UP and step == 4


def gather_kernel(
    chips, wg, lg, hg, wu, lu, hu, nt, ns, og, ou, nb,
    wv, lv, hv, ntv, nsv, xb, in_sem, send_sem, recv_sem, sib_sem, x_sem,
):
    f, z, core, to, sibling = position(chips)
    m = lax.axis_index("model")
    models = lax.axis_size("model")
    held = (og, ou, nb)
    barrier = pltpu.get_barrier_semaphore()
    for peer in (to[UP], to[DOWN], sibling):
        pl.semaphore_signal(
            barrier, inc=1, device_id={"fsdp": peer}, device_id_type=MESH
        )
    right, left = lax.rem(m + 1, models), lax.rem(m + models - 1, models)
    for peer in (right, left):
        pl.semaphore_signal(
            barrier, inc=1, device_id={"model": peer}, device_id_type=MESH
        )

    loads = []
    for k, (src, dst) in enumerate(
        (
            (lg, lv.at[0]), (hg, hv.at[0]), (wg, wv.at[0]), (nt, ntv), (ns, nsv),
            (lu, lv.at[1]), (hu, hv.at[1]), (wu, wv.at[1]),
        )
    ):
        load = pltpu.make_async_copy(src, dst, in_sem.at[k])
        load.start()
        loads.append(load)

    def push(kind, p, owner):
        ref = piece_of(held, kind, p, owner)
        copy_to(ref, ref, send_sem.at[2, kind], sib_sem.at[kind], sibling).start()

    def hop(way, step, kind, p, owner):
        ref = piece_of(held, kind, p, owner)
        place = ARRIVALS[way].index((step, kind, p))
        return copy_to(ref, ref, send_sem.at[way, kind], recv_sem.at[way, place], to[way])

    def send_own(way, kind, p):
        hop(way, 1, kind, p, f).start()

    def merge(kind, p):
        columns = rows_of(kind, p)
        low_high = lax.dot_general(
            lv[kind], hv[kind, :, columns], (((0,), (0,)), ((), ())),
            preferred_element_type=jnp.float32,
        )
        result = wv[kind, :, columns].astype(jnp.float32) + mix_rate * low_high
        piece_of(held, kind, p, f)[...] = result.T.astype(jnp.bfloat16)

    others = xb.at[pl.ds(0, models - 1)]
    lane = lax.broadcasted_iota(jnp.int32, (1, LANES), 1)
    part = LANES // models

    def norm_part():
        loads[3].wait()
        loads[4].wait()
        xb[m] = jnp.zeros((1, LANES), jnp.float32)
        xb[m, :, pl.ds(0, part)] = (ntv[...] + nsv[...]).reshape(1, part)

    def norm_send(owner, peer, k):
        pltpu.make_async_remote_copy(
            src_ref=xb.at[owner], dst_ref=xb.at[owner], send_sem=x_sem.at[0], recv_sem=x_sem.at[k],
            device_id={"model": peer}, device_id_type=MESH,
        ).start()

    def norm_arrived(k):
        pltpu.make_async_copy(xb.at[0], xb.at[0], x_sem.at[k]).wait()

    def norm_row():
        row = xb[0]
        for k in range(1, models):
            row = jnp.where(lane >= k * part, pltpu.roll(xb[k], k * part, 1), row)
        nb[f] = row

    made = [
        piece
        for pair in itertools.zip_longest(BLOCK[GATE], BLOCK[RISE])
        for piece in pair
        if piece
    ]

    def first_send(kind, p):
        send_own(UP if kind == GATE else DOWN, kind, p)
        push(kind, p, f)

    for k in (0, 1, 2):
        loads[k].wait()
    merge(*made[0])
    norm_part()
    for k in (5, 6, 7):
        loads[k].wait()
    merge(*made[1])
    merge(*made[2])
    pl.semaphore_wait(barrier, 5)
    norm_send(m, left, 1)
    norm_send(m, right, 2)
    first_send(*made[0])
    first_send(*made[1])
    for before, piece in zip(made[2:], made[3:]):
        merge(*piece)
        first_send(*before)
    for k in range(2, models - 1):
        norm_arrived(k)
        norm_send(lax.rem(m + models + 1 - k, models), right, k + 1)
    first_send(*made[-1])
    norm_arrived(1)
    norm_arrived(models - 1)
    norm_row()
    for way, kind in ((UP, RISE), (DOWN, GATE)):
        send_own(way, *BLOCK[kind][0])
        if way == UP:
            push(NORM, 0, f)
        send_own(way, NORM, 0)
        for piece in BLOCK[kind][1:]:
            send_own(way, *piece)
    pltpu.make_async_copy(others, others, x_sem.at[0]).wait()

    def take(c):
        sent = {way: list(ORDER) for way in (UP, DOWN)}
        pushed = list(ORDER)
        for i, way, step, kind, p in each(0, FIRST[c]):
            owner = owner_of(chips, z, core, way, step)
            hop(way, step, kind, p, owner).wait_recv()
            if step < HOPS[way][kind] and early(c, way, step + 1, kind, p):
                hop(way, step + 1, kind, p, owner).start()
                sent[way].append((kind, p))
            if shared_early(way, i):
                push(kind, p, owner)
                pushed.append((kind, p))
        for kind in (NORM, GATE, RISE):
            for way in (UP, DOWN):
                wait_for(held, kind, rows_in(sent[way])[kind], send_sem.at[way, kind])
            wait_for(held, kind, rows_in(pushed)[kind], send_sem.at[2, kind])
            wait_for(held, kind, rows_in(pushed)[kind], sib_sem.at[kind])

    for c in (0, 1):
        pl.when(core == c)(functools.partial(take, c))


def finish_kernel(chips, og, ou, nb, after, lg, lu, ln, send_sem, recv_sem, sib_sem, moved_sem, ready):
    f, z, core, to, sibling = position(chips)
    before, held = (og, ou, nb), (lg, lu, ln)
    barrier = pltpu.get_barrier_semaphore()
    for peer in (to[UP], to[DOWN]):
        pl.semaphore_signal(
            barrier, inc=1, device_id={"fsdp": peer}, device_id_type=MESH
        )

    @pl.when(core == AHEAD)
    def _():
        pl.semaphore_signal(
            barrier, inc=1, device_id={"fsdp": sibling}, device_id_type=MESH
        )
        pl.semaphore_wait(barrier, 2)

    @pl.when(core != AHEAD)
    def _():
        pl.semaphore_wait(barrier, 3)
        pl.semaphore_signal(
            ready, inc=1, device_id={"fsdp": sibling}, device_id_type=MESH
        )

    def push(source, kind, p, owner):
        copy_to(
            piece_of(source, kind, p, owner), piece_of(held, kind, p, owner),
            send_sem.at[2, kind], sib_sem.at[kind], sibling,
        ).start()

    def hop(source, way, step, kind, p, owner):
        place = ARRIVALS[way].index((step, kind, p))
        sem = send_sem.at[3, 0] if moved(way, step, kind, p) else send_sem.at[way, kind]
        return copy_to(
            piece_of(source, kind, p, owner), piece_of(held, kind, p, owner),
            sem, recv_sem.at[way, place], to[way],
        )

    last = chips - 1

    def moved_copy(source, owner):
        return copy_to(
            piece_of(source, *MOVED, owner), piece_of(held, *MOVED, owner),
            moved_sem.at[0], moved_sem.at[1], to[DOWN],
        )

    def forward(source, way, step, kind, p, owner, sent):
        if step < HOPS[way][kind]:
            copy = hop(source, way, step + 1, kind, p, owner)
            if moved(way, step + 1, kind, p):
                pl.when(z != last)(copy.start)
            else:
                copy.start()
                sent[way].append((kind, p))
        elif (kind, p) == MOVED and way == DOWN and step == 3:
            pl.when(z == 1)(moved_copy(source, owner).start)

    def take(c):
        sent = {way: [] for way in (UP, DOWN)}
        pushed, late = [], []
        for i, way, step, kind, p in each(0, FIRST[c]):
            owner = owner_of(chips, z, core, way, step)
            if step == HOPS[way][kind] or not early(c, way, step + 1, kind, p):
                forward(before, way, step, kind, p, owner, sent)
            if not shared_early(way, i):
                late.append((before, kind, p, way, step))

        def push_late():
            while late:
                source, kind, p, way, step = late.pop(0)
                push(source, kind, p, owner_of(chips, z, core, way, step))
                pushed.append((kind, p))

        met = c != AHEAD
        for i, way, step, kind, p in each(FIRST[c], COUNT):
            if not met and i >= MEET:
                pl.semaphore_wait(ready, 1)
                met = True
            if met:
                push_late()
            owner = owner_of(chips, z, core, way, step)
            if moved(way, step, kind, p):
                pl.when(z != 0)(hop(held, way, step, kind, p, owner).wait_recv)
                pl.when(z == 0)(moved_copy(held, owner).wait_recv)
            else:
                hop(held, way, step, kind, p, owner).wait_recv()
            forward(held, way, step, kind, p, owner, sent)
            late.append((held, kind, p, way, step))
        push_late()
        coming = [(kind, p) for _, _, _, kind, p in each(LEAST, COUNT)]
        if all(not early(c, UP, 4, *MOVED) for c in (0, 1)):
            unit = piece_of(held, *MOVED, f)
            kept = pltpu.make_async_copy(unit, unit, send_sem.at[3, 0])
            pl.when(z != last)(kept.wait)
            pl.when(z == 1)(moved_copy(held, f).wait_send)
        for kind in (NORM, GATE, RISE):
            for way in (UP, DOWN):
                wait_for(held, kind, rows_in(sent[way])[kind], send_sem.at[way, kind])
            wait_for(held, kind, rows_in(pushed)[kind], send_sem.at[2, kind])
            wait_for(held, kind, rows_in(coming)[kind], sib_sem.at[kind])

    for c in (0, 1):
        pl.when(core == c)(functools.partial(take, c))


def runs(pieces):
    out = []
    for kind, p in sorted(pieces):
        start, size = sum(CUTS[kind][:p]), CUTS[kind][p]
        if out and out[-1][0] == kind and sum(out[-1][1:]) == start:
            out[-1] = (kind, out[-1][1], out[-1][2] + size)
        else:
            out.append((kind, start, size))
    return out


def store(chips, z, core, c, held, final, sem, sides, own):
    total = [0, 0]
    for mine, (first, last) in ((False, sides[1]), (True, sides[0])):
        line = core if mine else 1 - core
        blocks = {}
        for _, way, step, kind, p in each(first, last):
            if kind != NORM:
                blocks.setdefault((way, step), []).append((kind, p))
        if own:
            blocks[UP, 0] = [piece for piece in ORDER if piece[0] != NORM]
        for (way, step), pieces in blocks.items():
            lanes = lanes_of(owner_of(chips, z, line, way, step))
            for kind, start, size in runs(pieces):
                at = (pl.ds(start, size), lanes)
                pltpu.make_async_copy(held[kind].at[at], final[kind].at[at], sem.at[kind]).start()
                total[kind] += size
    return total


def write_kernel(chips, og, ou, fg, fu, after, sem):
    _, z, core, _, _ = position(chips)
    after[...] = jnp.zeros_like(after)
    held, final = (og, ou), (fg, fu)

    def take(c):
        total = store(chips, z, core, c, held, final, sem, ((0, FIRST[c]), (0, LEAST)), True)
        for kind in (GATE, RISE):
            wait_for(held, kind, total[kind], sem.at[kind])

    for c in (0, 1):
        pl.when(core == c)(functools.partial(take, c))


def write_rest_kernel(chips, fg_in, fu_in, nb, lg, lu, ln, fg, fu, fn, rows, norm, sem):
    f, z, core, _, sibling = position(chips)
    held, final = (lg, lu), (fg, fu)

    def take(c):
        total = store(
            chips, z, core, c, held, final, sem, ((FIRST[c], COUNT), (LEAST, COUNT)), False
        )
        rows[f] = nb[f]
        rows[sibling] = nb[sibling]
        for i, way, step, kind, p in each(0, COUNT):
            if kind == NORM:
                for line, source in ((core, i < FIRST[c]), (1 - core, i < LEAST)):
                    owner = owner_of(chips, z, line, way, step)
                    rows[owner] = nb[owner] if source else ln[owner]
        norm[...] = rows[...].reshape(norm.shape).astype(norm.dtype)
        last = pltpu.make_async_copy(norm, fn, sem.at[2])
        last.start()
        for kind in (GATE, RISE):
            wait_for(held, kind, total[kind], sem.at[kind])
        last.wait()

    for c in (0, 1):
        pl.when(core == c)(functools.partial(take, c))


def solution(mesh):
    fsdp = mesh.shape["fsdp"]
    models = mesh.shape["model"]
    chips = fsdp // 2

    def body(wg, lg, hg, wu, lu, hu, nt, ns):
        depth, width = wg.shape
        rank = lg.shape[1]
        model_width = depth * fsdp
        anywhere = pl.BlockSpec(memory_space=pl.ANY)
        on_chip = pl.BlockSpec(memory_space=pltpu.VMEM)
        final = jax.ShapeDtypeStruct((width, model_width), jnp.bfloat16)
        on_chip_held = (
            pltpu.VMEM((width, model_width), jnp.bfloat16),
            pltpu.VMEM((width, model_width), jnp.bfloat16),
            pltpu.VMEM((fsdp, 1, LANES), jnp.float32),
        )
        ring_sems = [
            pltpu.SemaphoreType.DMA((4, 3)),
            pltpu.SemaphoreType.DMA((2, COUNT)),
            pltpu.SemaphoreType.DMA((3,)),
        ]
        og, ou, nb = pl.pallas_call(
            functools.partial(gather_kernel, chips),
            out_shape=on_chip_held,
            in_specs=[pl.BlockSpec(memory_space=pltpu.HBM)] * 8,
            out_specs=(on_chip,) * 3,
            scratch_shapes=[
                pltpu.VMEM((2, depth, width), jnp.bfloat16),
                pltpu.VMEM((2, rank, depth), jnp.bfloat16),
                pltpu.VMEM((2, rank, width), jnp.bfloat16),
                pltpu.VMEM(nt.shape, jnp.float32),
                pltpu.VMEM(ns.shape, jnp.float32),
                pltpu.VMEM((models, 1, LANES), jnp.float32),
                pltpu.SemaphoreType.DMA((8,)),
                *ring_sems,
                pltpu.SemaphoreType.DMA((models,)),
            ],
            compiler_params=pltpu.CompilerParams(
                collective_id=0, has_side_effects=True, vmem_limit_bytes=50257920
            ),
            name="gather",
        )(wg, lg.T, hg, wu, lu.T, hu, nt, ns)
        fg, fu, after = pl.pallas_call(
            functools.partial(write_kernel, chips),
            out_shape=(final, final, pltpu.VMEM((8, LANES), jnp.float32)),
            in_specs=[on_chip] * 2,
            out_specs=(anywhere, anywhere, on_chip),
            scratch_shapes=[pltpu.SemaphoreType.DMA((2,))],
            compiler_params=pltpu.CompilerParams(vmem_limit_bytes=4 << 20),
            name="write",
        )(og, ou)
        lg2, lu2, ln = pl.pallas_call(
            functools.partial(finish_kernel, chips),
            out_shape=on_chip_held,
            in_specs=[on_chip] * 4,
            out_specs=(on_chip,) * 3,
            scratch_shapes=[
                *ring_sems, pltpu.SemaphoreType.DMA((2,)), pltpu.SemaphoreType.REGULAR
            ],
            compiler_params=pltpu.CompilerParams(
                collective_id=1, has_side_effects=True, vmem_limit_bytes=4 << 20
            ),
            name="finish",
        )(og, ou, nb, after)
        fg, fu, fn = pl.pallas_call(
            functools.partial(write_rest_kernel, chips),
            out_shape=(final, final, jax.ShapeDtypeStruct((fsdp, LANES), jnp.bfloat16)),
            in_specs=[anywhere] * 2 + [on_chip] * 4,
            out_specs=(anywhere,) * 3,
            scratch_shapes=[
                pltpu.VMEM((fsdp, 1, LANES), jnp.float32),
                pltpu.VMEM((fsdp, LANES), jnp.bfloat16),
                pltpu.SemaphoreType.DMA((3,)),
            ],
            input_output_aliases={0: 0, 1: 1},
            compiler_params=pltpu.CompilerParams(vmem_limit_bytes=4 << 20),
            name="write_rest",
        )(fg, fu, nb, lg2, lu2, ln)
        return fg, fu, fn.reshape(fsdp * LANES)

    return jax.shard_map(
        body,
        mesh=mesh,
        in_specs=(
            P(("ens", "fsdp"), "model"),
            P(("ens", "fsdp"), None),
            P("ens", "model"),
            P(("ens", "fsdp"), "model"),
            P(("ens", "fsdp"), None),
            P("ens", "model"),
            P(("ens", "fsdp", "model")),
            P(("ens", "fsdp", "model")),
        ),
        out_specs=(P(("ens", "model"), None), P(("ens", "model"), None), P("ens")),
        check_vma=False,
    )
```
